16 devices in a mesh: dp: 2 (over y, z), ep: 8 (over x, core).
Axes of the slice: x: 4, y: 2, z: 1, core: 2. Of those that a mesh axis runs over, the one named last changes fastest.
The devices are a block of a 4x4x8 slice.
Arguments:
- hidden: bfloat16 [16, 128, 1024], P(('dp', 'ep')), parts along dimension 0
- expert_ids: int32 [16, 128, 8], P(('dp', 'ep')), parts along dimension 0
- slot_ids: int32 [16, 128, 8], P(('dp', 'ep')), parts along dimension 0
- attn_norm: bfloat16 [1024], replicated
- w_query: bfloat16 [1024, 1024], replicated
- w_key: bfloat16 [1024, 512], replicated
- w_value: bfloat16 [1024, 512], replicated
- w_out: bfloat16 [16, 64, 1024], replicated
- ffn_norm: bfloat16 [1024], replicated
- ffn_gate: bfloat16 [1024, 4096], replicated
- ffn_up: bfloat16 [1024, 4096], replicated
- ffn_down: bfloat16 [4096, 1024], replicated
- moe_norm: bfloat16 [1024], replicated
- w_router: bfloat16 [1024, 32], replicated
- exp_gate: bfloat16 [32, 1024, 512], P('ep')
- exp_up: bfloat16 [32, 1024, 512], P('ep')
- exp_down: bfloat16 [32, 512, 1024], P('ep')
Outputs:
- output: bfloat16 [16, 128, 1024], P(('dp', 'ep')), parts along dimension 0
There are 2 independent parts. The reference program is written for one: setup_inputs(seed, part) draws one part's arguments, and reference() takes and returns one part's arrays. A program takes and returns all parts, laid end to end along the dimension named above; an argument that names none is the same for every part.
All inputs are finite; a program needn't handle non-finite values.
Results may differ from the reference program's by a relative error of at most 0.00945966.
Values are sent between devices in bfloat16 or wider.
A program may use at most 768 MiB of HBM per device.

```python
import jax
import jax.numpy as jnp
from jax import lax

D_MODEL = 1024
N_HEADS = 16
KV_HEADS = 8
HEAD_DIM = 64
FF_DIM = 4096
N_EXPERTS = 32
TOP_K = 8
EXPERT_FF = 512
SEQ_LEN = 128
BATCH_DEV = 1
GROUP_SIZE = 8

N_SEQS = GROUP_SIZE * BATCH_DEV
TOKENS_DEV = BATCH_DEV * SEQ_LEN
TOKENS = GROUP_SIZE * TOKENS_DEV
LOCAL_EXPERTS = N_EXPERTS // GROUP_SIZE
CAPACITY = 3 * TOKENS_DEV * TOP_K // N_EXPERTS
HOT_DEVICES = max(1, GROUP_SIZE // 8)
Q_PER_KV = N_HEADS // KV_HEADS
RMS_EPS = 1e-6
ROPE_BASE = 10000.0


def draw_routing(route_key):
    key_devs, key_rows = jax.random.split(route_key)
    mean_load = TOKENS_DEV * TOP_K // N_EXPERTS
    hot_count = HOT_DEVICES * LOCAL_EXPERTS
    cold_count = N_EXPERTS - hot_count
    cold_total = N_EXPERTS * mean_load - hot_count * CAPACITY
    cold_base = cold_total // cold_count
    cold_extra = cold_total - cold_base * cold_count
    expert_rank = jnp.arange(N_EXPERTS, dtype=jnp.int32)
    rank_load = jnp.where(expert_rank < hot_count, CAPACITY, cold_base + (expert_rank - hot_count < cold_extra).astype(jnp.int32))
    rank_start = jnp.cumsum(rank_load) - rank_load
    copy_rank = jnp.repeat(expert_rank, rank_load, total_repeat_length=TOKENS_DEV * TOP_K)
    copy_slot = jnp.arange(TOKENS_DEV * TOP_K, dtype=jnp.int32) - rank_start[copy_rank]
    dev_order = jax.random.permutation(key_devs, GROUP_SIZE)
    expert_of_rank = (dev_order[:, None] * LOCAL_EXPERTS + jnp.arange(LOCAL_EXPERTS)[None, :]).reshape(N_EXPERTS)
    base_ids = expert_of_rank[copy_rank].reshape(TOP_K, TOKENS_DEV).T
    base_slots = copy_slot.reshape(TOP_K, TOKENS_DEV).T

    def one_device(dev_key):
        key_perm, key_shift = jax.random.split(dev_key)
        row_order = jax.random.permutation(key_perm, TOKENS_DEV)
        col_shift = jax.random.randint(key_shift, (TOKENS_DEV, 1), 0, TOP_K)
        col_index = (jnp.arange(TOP_K)[None, :] + col_shift) % TOP_K
        dev_ids = jnp.take_along_axis(base_ids[row_order], col_index, axis=1)
        dev_slots = jnp.take_along_axis(base_slots[row_order], col_index, axis=1)
        return dev_ids, dev_slots

    dev_ids, dev_slots = jax.vmap(one_device)(jax.random.split(key_rows, GROUP_SIZE))
    return (dev_ids.astype(jnp.int32).reshape(N_SEQS, SEQ_LEN, TOP_K), dev_slots.astype(jnp.int32).reshape(N_SEQS, SEQ_LEN, TOP_K))


def draw_normal(draw_key, shape, std):
    return (jax.random.normal(draw_key, shape, jnp.float32) * std).astype(jnp.bfloat16)


def draw_gain(gain_key):
    return (1.0 + 0.4 * jax.random.normal(gain_key, (D_MODEL,), jnp.float32)).astype(jnp.bfloat16)


def setup_inputs(seed: int = 0, part: int = 0) -> dict:
    shared = jax.random.split(jax.random.key(seed), 14)
    part_key = jax.random.fold_in(jax.random.key(seed + 1), part)
    expert_ids, slot_ids = draw_routing(jax.random.fold_in(part_key, 3))
    q_width = N_HEADS * HEAD_DIM
    kv_width = KV_HEADS * HEAD_DIM
    return {
        'hidden': draw_normal(jax.random.fold_in(part_key, 1), (N_SEQS, SEQ_LEN, D_MODEL), 1.0),
        'expert_ids': expert_ids,
        'slot_ids': slot_ids,
        'attn_norm': draw_gain(shared[0]),
        'w_query': draw_normal(shared[1], (D_MODEL, q_width), 2.0 * D_MODEL ** -0.5),
        'w_key': draw_normal(shared[2], (D_MODEL, kv_width), D_MODEL ** -0.5),
        'w_value': draw_normal(shared[3], (D_MODEL, kv_width), D_MODEL ** -0.5),
        'w_out': draw_normal(shared[4], (N_HEADS, HEAD_DIM, D_MODEL), 2.0 * q_width ** -0.5),
        'ffn_norm': draw_gain(shared[5]),
        'ffn_gate': draw_normal(shared[6], (D_MODEL, FF_DIM), D_MODEL ** -0.5),
        'ffn_up': draw_normal(shared[7], (D_MODEL, FF_DIM), D_MODEL ** -0.5),
        'ffn_down': draw_normal(shared[8], (FF_DIM, D_MODEL), FF_DIM ** -0.5),
        'moe_norm': draw_gain(shared[9]),
        'w_router': draw_normal(shared[10], (D_MODEL, N_EXPERTS), 1.5 * D_MODEL ** -0.5),
        'exp_gate': draw_normal(shared[11], (N_EXPERTS, D_MODEL, EXPERT_FF), D_MODEL ** -0.5),
        'exp_up': draw_normal(shared[12], (N_EXPERTS, D_MODEL, EXPERT_FF), D_MODEL ** -0.5),
        'exp_down': draw_normal(shared[13], (N_EXPERTS, EXPERT_FF, D_MODEL), 2.0 * EXPERT_FF ** -0.5),
    }


def rms_norm(row_vals, norm_scale):
    as_float = row_vals.astype(jnp.float32)
    inv_rms = lax.rsqrt(jnp.mean(as_float * as_float, axis=-1, keepdims=True) + RMS_EPS)
    return (as_float * inv_rms * norm_scale.astype(jnp.float32)).astype(jnp.bfloat16)


def rotary(head_vals):
    half_dim = HEAD_DIM // 2
    inv_freq = ROPE_BASE ** (-2.0 * jnp.arange(half_dim, dtype=jnp.float32) / HEAD_DIM)
    angles = jnp.arange(SEQ_LEN, dtype=jnp.float32)[:, None] * inv_freq[None, :]
    cos_t = jnp.cos(angles)[:, None, :]
    sin_t = jnp.sin(angles)[:, None, :]
    first_half = head_vals[..., :half_dim]
    second_half = head_vals[..., half_dim:]
    return jnp.concatenate([first_half * cos_t - second_half * sin_t, second_half * cos_t + first_half * sin_t], axis=-1)


def reference(hidden, expert_ids, slot_ids, attn_norm, w_query, w_key, w_value, w_out, ffn_norm, ffn_gate, ffn_up, ffn_down, moe_norm, w_router, exp_gate, exp_up, exp_down):
    causal = jnp.arange(SEQ_LEN)[:, None] >= jnp.arange(SEQ_LEN)[None, :]
    out_mat = w_out.reshape(N_HEADS * HEAD_DIM, D_MODEL)

    def dense_seq(seq_rows):
        normed = rms_norm(seq_rows, attn_norm)
        queries = rotary(jnp.dot(normed, w_query, preferred_element_type=jnp.float32).reshape(SEQ_LEN, N_HEADS, HEAD_DIM)).astype(jnp.bfloat16)
        key_vals = rotary(jnp.dot(normed, w_key, preferred_element_type=jnp.float32).reshape(SEQ_LEN, KV_HEADS, HEAD_DIM)).astype(jnp.bfloat16)
        values = jnp.dot(normed, w_value, preferred_element_type=jnp.float32).astype(jnp.bfloat16).reshape(SEQ_LEN, KV_HEADS, HEAD_DIM)
        grouped = queries.reshape(SEQ_LEN, KV_HEADS, Q_PER_KV, HEAD_DIM)
        scores = jnp.einsum('sgrd,tgd->grst', grouped.astype(jnp.float32), key_vals.astype(jnp.float32)) * HEAD_DIM ** -0.5
        scores = jnp.where(causal, scores, -jnp.inf)
        attn_prob = jax.nn.softmax(scores, axis=-1).astype(jnp.bfloat16)
        context = jnp.einsum('grst,tgd->sgrd', attn_prob.astype(jnp.float32), values.astype(jnp.float32)).astype(jnp.bfloat16)
        attn_out = (seq_rows.astype(jnp.float32) + jnp.dot(context.reshape(SEQ_LEN, N_HEADS * HEAD_DIM), out_mat, preferred_element_type=jnp.float32)).astype(jnp.bfloat16)
        normed_ffn = rms_norm(attn_out, ffn_norm)
        hidden_act = (jax.nn.silu(jnp.dot(normed_ffn, ffn_gate, preferred_element_type=jnp.float32)) * jnp.dot(normed_ffn, ffn_up, preferred_element_type=jnp.float32)).astype(jnp.bfloat16)
        return attn_out.astype(jnp.float32) + jnp.dot(hidden_act, ffn_down, preferred_element_type=jnp.float32)

    dense_out = lax.map(dense_seq, hidden).reshape(TOKENS, D_MODEL)

    token_rows = hidden.reshape(TOKENS, D_MODEL)
    choice_ids = expert_ids.reshape(TOKENS, TOP_K)
    choice_slots = slot_ids.reshape(TOKENS, TOP_K)
    normed = rms_norm(token_rows, moe_norm)
    logits = jnp.dot(normed, w_router, preferred_element_type=jnp.float32)
    gate_vals = jax.nn.softmax(jnp.take_along_axis(logits, choice_ids, axis=1), axis=-1)
    src_dev = jnp.arange(TOKENS, dtype=jnp.int32) // TOKENS_DEV
    buf_pos = (choice_ids * GROUP_SIZE + src_dev[:, None]) * CAPACITY + choice_slots
    buf_rows = N_EXPERTS * GROUP_SIZE * CAPACITY
    owner_copy = jnp.full((buf_rows,), TOKENS * TOP_K, jnp.int32).at[buf_pos.reshape(-1)].set(jnp.arange(TOKENS * TOP_K, dtype=jnp.int32))
    padded = jnp.concatenate([normed, jnp.zeros((1, D_MODEL), jnp.bfloat16)], axis=0)
    gate_ext = jnp.concatenate([gate_vals.reshape(-1), jnp.zeros((1,), jnp.float32)])

    def one_expert(moe_acc, operands):
        copy_index, gate_w, up_w, down_w = operands
        token_index = copy_index // TOP_K
        expert_rows = padded[token_index]
        z_gate = jnp.dot(expert_rows, gate_w, preferred_element_type=jnp.float32)
        z_up = jnp.dot(expert_rows, up_w, preferred_element_type=jnp.float32)
        hidden_act = (jax.nn.silu(z_gate) * z_up).astype(jnp.bfloat16)
        expert_y = jnp.dot(hidden_act, down_w, preferred_element_type=jnp.float32).astype(jnp.bfloat16)
        weighted = gate_ext[copy_index][:, None] * expert_y.astype(jnp.float32)
        return moe_acc.at[token_index].add(weighted), None

    moe_acc = lax.scan(one_expert, jnp.zeros((TOKENS + 1, D_MODEL), jnp.float32), (owner_copy.reshape(N_EXPERTS, GROUP_SIZE * CAPACITY), exp_gate, exp_up, exp_down))[0]
    moe_out = moe_acc[:TOKENS]
    return (dense_out + moe_out).astype(jnp.bfloat16).reshape(N_SEQS, SEQ_LEN, D_MODEL)
```

```python
import functools

import jax
import jax.numpy as jnp
import numpy as np
from jax import lax
from jax.experimental import pallas as pl
from jax.experimental.pallas import tpu as pltpu
from jax.sharding import PartitionSpec as P

RMS_EPS = 1e-6
ROPE_BASE = 10000.0
MESH = pl.DeviceIdType.MESH
F32, BF16 = jnp.float32, jnp.bfloat16
LANES = 128
FF_BLOCK = 512
COL = 256


def rms_rows(row_vals, norm_scale):
    as_float = row_vals.astype(F32)
    inv_rms = lax.rsqrt(jnp.mean(as_float * as_float, axis=-1, keepdims=True) + RMS_EPS)
    return (as_float * inv_rms * norm_scale.astype(F32)).astype(BF16)


def silu(z):
    return z / (1.0 + jnp.exp(-z))


def dot(a, b):
    return jnp.dot(a, b, preferred_element_type=F32)


def rope_tables(seq_len, head_dim):
    half = head_dim // 2
    lane = np.arange(LANES)
    freq = ROPE_BASE ** (-2.0 * (lane % half) / head_dim)
    angle = np.arange(seq_len)[:, None] * freq[None, :]
    sign = np.where(lane % head_dim < half, -1.0, 1.0)
    return np.cos(angle).astype(np.float32), (np.sin(angle) * sign[None, :]).astype(np.float32)


def kernel(group, hidden, ids, attn_norm, w_query, w_key, w_value, w_out, ffn_norm, ffn_gate, ffn_up, ffn_down,
           moe_norm, w_router, exp_gate, exp_up, exp_down, cos_t, sin_t, out,
           v_hid, v_ids, v_an, v_wq, v_wk, v_wv, v_wo, v_fn, v_fg, v_fu, v_fd, v_mn, v_wr, v_eg, v_eu, v_ed, v_cos, v_sin,
           v_out, x_buf, g_buf, p_buf, pr_buf, tb, rb, qf, kf, vf, ctx, hb, att, ffn_acc,
           w_sem, s_sem, r_sem):
    tokens, model = v_hid.shape
    half = tokens // 2
    n_local = v_eg.shape[0]
    exp_ff = v_eg.shape[2]
    ff_dim = v_fg.shape[1]
    me = lax.axis_index('ep')
    partner = me + 1 - 2 * lax.rem(me, 2)
    right = lax.rem(me + 2, group)
    left = lax.rem(me + group - 2, group)

    loads = {}

    def load(name, src, dst):
        loads[name] = pltpu.make_async_copy(src, dst, w_sem.at[len(loads)])
        loads[name].start()

    def ready(*names):
        for name in names:
            loads[name].wait()

    copies = {}

    def remote(name, src, dst, device):
        k = len(copies)
        copies[name] = pltpu.make_async_remote_copy(
            src_ref=src, dst_ref=dst, send_sem=s_sem.at[k], recv_sem=r_sem.at[k],
            device_id={'ep': device}, device_id_type=MESH)
        return copies[name]

    def send(*names):
        for name in names:
            copies[name].start()

    def recv(*names):
        for name in names:
            copies[name].wait_recv()

    lo, hi, al, ot = pl.ds(0, half), pl.ds(half, half), pl.ds(0, tokens), pl.ds(tokens, tokens)
    remote('a1', x_buf.at[0, lo], x_buf.at[1, lo], right)
    remote('a2', x_buf.at[0, hi], x_buf.at[1, hi], left)
    remote('a3', x_buf.at[0, hi], x_buf.at[2, hi], right)
    remote('a4', x_buf.at[0, lo], x_buf.at[2, lo], left)
    remote('f1', x_buf.at[1, lo], x_buf.at[3, lo], right)
    remote('f2', x_buf.at[1, hi], x_buf.at[3, hi], left)
    for c in range(4):
        remote(f'd{c}', x_buf.at[c, al], x_buf.at[c, ot], partner)
    remote('g1', g_buf.at[0, 0], g_buf.at[1, 0], right)
    remote('g2', g_buf.at[0, 0], g_buf.at[2, 0], left)
    remote('g3', g_buf.at[1, 0], g_buf.at[3, 0], right)
    for c in range(4):
        remote(f'gd{c}', g_buf.at[c, 0], g_buf.at[c, 1], partner)
    for c in range(4):
        remote(f'p{c}', p_buf.at[c, ot], pr_buf.at[c], partner)
    remote('i1', p_buf.at[1, hi], rb.at[1, hi], right)
    remote('i2', p_buf.at[1, lo], rb.at[0, lo], left)
    remote('o1', p_buf.at[3, lo], tb.at[lo], right)
    remote('o2', p_buf.at[3, hi], tb.at[hi], left)
    remote('w1', p_buf.at[2, lo], rb.at[1, lo], right)
    remote('w2', p_buf.at[2, hi], rb.at[0, hi], left)

    load('hid', hidden, v_hid)
    load('mn', moe_norm, v_mn)
    load('wr', w_router, v_wr)
    load('ids', ids, v_ids)
    load('an', attn_norm, v_an)
    load('wq', w_query, v_wq)
    load('wk', w_key, v_wk)
    load('wv', w_value, v_wv)
    load('cos', cos_t, v_cos)
    load('sin', sin_t, v_sin)

    barrier = pltpu.get_barrier_semaphore()
    for peer in (partner, left, right):
        pl.semaphore_signal(barrier, inc=1, device_id={'ep': peer}, device_id_type=MESH)

    for e in range(n_local):
        load(f'eg{e}', exp_gate.at[e], v_eg.at[e])
        load(f'eu{e}', exp_up.at[e], v_eu.at[e])
        load(f'ed{e}', exp_down.at[e], v_ed.at[e])
    load('wo', w_out, v_wo)
    load('fn', ffn_norm, v_fn)

    ready('hid', 'mn')
    x_buf[0, :tokens] = rms_rows(v_hid[...], v_mn[...])
    pl.semaphore_wait(barrier, 3)
    send('a1', 'a2', 'a3', 'a4', 'd0')

    ready('wr', 'ids')
    logits = dot(x_buf[0, :tokens], v_wr[...])
    n_experts = logits.shape[1]
    chosen = lax.broadcasted_iota(jnp.int32, logits.shape, 1)
    mask = jnp.zeros(logits.shape, jnp.bool_)
    id_vals = v_ids[...]
    for j in range(id_vals.shape[1]):
        mask = jnp.logical_or(mask, chosen == id_vals[:, j:j + 1])
    top = jnp.max(jnp.where(mask, logits, -jnp.inf), axis=-1, keepdims=True)
    powers = jnp.where(mask, jnp.exp(logits - top), 0.0)
    gates = powers / jnp.sum(powers, axis=-1, keepdims=True)
    g_buf[0, 0] = gates.T
    send('g1', 'g2', 'gd0')

    ready('an', 'wq', 'wk', 'wv', 'cos', 'sin')
    normed = rms_rows(v_hid[...], v_an[...])
    qf[...] = dot(normed, v_wq[...])
    kf[...] = dot(normed, v_wk[...])
    vf[...] = dot(normed, v_wv[...])

    recv('a1', 'a2')
    send('f1', 'f2', 'd1')
    recv('g1', 'g2')
    send('g3', 'gd1', 'gd2')

    n_blk = ff_dim // 1024
    for b in range(n_blk):
        cols = pl.ds(b * 1024, 1024)
        load(f'fg{b}', ffn_gate.at[:, cols], v_fg.at[:, cols])
        load(f'fu{b}', ffn_up.at[:, cols], v_fu.at[:, cols])
        load(f'fd{b}', ffn_down.at[cols], v_fd.at[cols])

    lane = lax.broadcasted_iota(jnp.int32, (tokens, LANES), 1)
    low_half = lax.rem(lane, 64) < 32
    head0 = lane < 64
    cos_v, sin_v = v_cos[...], v_sin[...]

    def rope(x):
        swapped = jnp.where(low_half, pltpu.roll(x, LANES - 32, 1), pltpu.roll(x, 32, 1))
        return x * cos_v + swapped * sin_v

    row = lax.rem(lax.broadcasted_iota(jnp.int32, (2 * tokens, tokens), 0), tokens)
    causal = row >= lax.broadcasted_iota(jnp.int32, (2 * tokens, tokens), 1)
    for t in range(kf.shape[1] // LANES):
        kt = rope(kf[:, t * LANES:(t + 1) * LANES])
        vt = vf[:, t * LANES:(t + 1) * LANES]
        kt_r, vt_r = pltpu.roll(kt, 64, 1), pltpu.roll(vt, 64, 1)
        for s in range(2):
            g = 2 * t + s
            k2 = (jnp.where(head0, kt, kt_r) if s == 0 else jnp.where(head0, kt_r, kt)).astype(BF16)
            v2 = (jnp.where(head0, vt, vt_r) if s == 0 else jnp.where(head0, vt_r, vt)).astype(BF16)
            q = rope(qf[:, g * LANES:(g + 1) * LANES])
            q2 = jnp.concatenate([jnp.where(head0, q, 0.0), jnp.where(head0, 0.0, q)], axis=0).astype(BF16)
            scores = lax.dot_general(q2, k2, (((1,), (1,)), ((), ())), preferred_element_type=F32) * 64 ** -0.5
            scores = jnp.where(causal, scores, -jnp.inf)
            prob = jnp.exp(scores - jnp.max(scores, axis=-1, keepdims=True))
            prob = (prob / jnp.sum(prob, axis=-1, keepdims=True)).astype(BF16)
            both = dot(prob, v2)
            ctx[:, g * LANES:(g + 1) * LANES] = jnp.where(head0, both[:tokens], both[tokens:]).astype(BF16)

    recv('a3', 'a4')
    send('d2')

    e_lane = lax.broadcasted_iota(jnp.int32, (2 * tokens, n_experts), 1) - me * n_local
    t_lane = lax.broadcasted_iota(jnp.int32, (n_experts, tokens), 1) < half

    def chunk_gates(c):
        parts = []
        for par in range(2):
            if c == 0:
                gt = g_buf[0, par]
            elif c == 3:
                gt = g_buf[3, par]
            elif c == 1:
                gt = jnp.where(t_lane, g_buf[1, par], g_buf[2, par])
            else:
                gt = jnp.where(t_lane, g_buf[2, par], g_buf[1, par])
            parts.append(gt.T)
        return jnp.concatenate(parts, axis=0)

    def expert(c, e, gates_c):
        gate = jnp.sum(jnp.where(e_lane == e, gates_c, 0.0), axis=-1, keepdims=True)
        used = gate > 0.0
        x = x_buf[c]
        for n in range(exp_ff // COL):
            cols = slice(n * COL, (n + 1) * COL)
            act = silu(dot(x, v_eg[e, :, cols])) * dot(x, v_eu[e, :, cols])
            hb[:, cols] = jnp.where(used, act, 0.0).astype(BF16)
        h = hb[...]
        for n in range(model // COL):
            cols = slice(n * COL, (n + 1) * COL)
            y = gate * dot(h, v_ed[e, :, cols]).astype(BF16).astype(F32)
            p_buf[c, :, cols] = y if e == 0 else p_buf[c, :, cols] + y

    def ffn_block(b, x):
        act_cols = slice(b * FF_BLOCK, (b + 1) * FF_BLOCK)
        for n in range(FF_BLOCK // COL):
            cols = slice(b * FF_BLOCK + n * COL, b * FF_BLOCK + (n + 1) * COL)
            act = silu(dot(x, v_fg[:, cols])) * dot(x, v_fu[:, cols])
            hb[:tokens, n * COL:(n + 1) * COL] = act.astype(BF16)
        h = hb[:tokens]
        for n in range(model // COL):
            cols = slice(n * COL, (n + 1) * COL)
            y = dot(h, v_fd[act_cols, cols])
            ffn_acc[:, cols] = y + (att[:, cols].astype(F32) if b == 0 else ffn_acc[:, cols])

    def add_partner(c):
        recv(f'p{c}')
        p_buf[c, :tokens] = p_buf[c, :tokens] + pr_buf[c]

    for e in range(n_local):
        ready(f'eg{e}', f'eu{e}', f'ed{e}')

    recv('d1', 'gd1', 'gd2')
    g = chunk_gates(1)
    expert(1, 0, g)
    expert(1, 1, g)
    recv('f1', 'f2', 'g3')
    send('d3', 'gd3')
    expert(1, 2, g)
    expert(1, 3, g)
    send('p1')
    recv('d3', 'gd3')
    g = chunk_gates(3)
    expert(3, 0, g)
    expert(3, 1, g)
    add_partner(1)
    send('i1', 'i2')
    expert(3, 2, g)
    expert(3, 3, g)
    send('p3')
    recv('d2')
    g = chunk_gates(2)
    expert(2, 0, g)
    expert(2, 1, g)
    add_partner(3)
    send('o1', 'o2')
    expert(2, 2, g)
    expert(2, 3, g)
    send('p2')
    recv('d0', 'gd0')
    g = chunk_gates(0)
    expert(0, 0, g)
    expert(0, 1, g)
    add_partner(2)
    expert(0, 2, g)
    expert(0, 3, g)
    send('p0')

    ready('wo', 'fn')
    att[...] = (v_hid[...].astype(F32) + dot(ctx[...], v_wo[...])).astype(BF16)
    normed_ffn = rms_rows(att[...], v_fn[...])
    for b in range(ff_dim // FF_BLOCK):
        if (b * FF_BLOCK) % 1024 == 0:
            i = b * FF_BLOCK // 1024
            ready(f'fg{i}', f'fu{i}', f'fd{i}')
        ffn_block(b, normed_ffn)
        if b == 2:
            recv('o1')
            p_buf[2, :half] = p_buf[2, :half] + tb[:half]
            send('w1')
            recv('o2')
            p_buf[2, half:tokens] = p_buf[2, half:tokens] + tb[half:]
            send('w2')
    add_partner(0)
    ffn_acc[...] = ffn_acc[...] + p_buf[0, :tokens]
    recv('i1', 'i2', 'w1', 'w2')
    v_out[...] = (ffn_acc[...] + rb[0] + rb[1]).astype(BF16)
    done = pltpu.make_async_copy(v_out, out, w_sem.at[len(loads)])
    done.start()
    for copy in copies.values():
        copy.wait_send()
    done.wait()


def solution(mesh):
    group = mesh.shape['ep']
    row_spec = P(('dp', 'ep'), None, None)
    vec_spec = P(None)
    mat_spec = P(None, None)
    cube_spec = P(None, None, None)
    expert_spec = P('ep', None, None)

    def per_device(hidden, expert_ids, slot_ids, attn_norm, w_query, w_key, w_value, w_out, ffn_norm, ffn_gate, ffn_up, ffn_down, moe_norm, w_router, exp_gate, exp_up, exp_down):
        n_seqs, seq_len, model = hidden.shape
        tokens = n_seqs * seq_len
        n_heads, head_dim = w_out.shape[0], w_out.shape[1]
        top_k = expert_ids.shape[-1]
        n_local, _, exp_ff = exp_gate.shape
        n_experts = w_router.shape[1]
        kv_dim = w_key.shape[1]
        assert n_seqs == 1 and group == 8 and head_dim == 64
        cos_t, sin_t = rope_tables(seq_len, head_dim)
        args = (hidden.reshape(tokens, model), expert_ids.reshape(tokens, top_k), attn_norm.reshape(1, model),
                w_query, w_key, w_value, w_out.reshape(n_heads * head_dim, model), ffn_norm.reshape(1, model),
                ffn_gate, ffn_up, ffn_down, moe_norm.reshape(1, model), w_router, exp_gate, exp_up, exp_down,
                jnp.asarray(cos_t), jnp.asarray(sin_t))
        vmem = [pltpu.VMEM(a.shape, a.dtype) for a in args]
        scratch = vmem + [
            pltpu.VMEM((tokens, model), BF16),
            pltpu.VMEM((4, 2 * tokens, model), BF16),
            pltpu.VMEM((4, 2, n_experts, tokens), F32),
            pltpu.VMEM((4, 2 * tokens, model), F32),
            pltpu.VMEM((4, tokens, model), F32),
            pltpu.VMEM((tokens, model), F32),
            pltpu.VMEM((2, tokens, model), F32),
            pltpu.VMEM((tokens, n_heads * head_dim), F32),
            pltpu.VMEM((tokens, kv_dim), F32),
            pltpu.VMEM((tokens, kv_dim), F32),
            pltpu.VMEM((tokens, n_heads * head_dim), BF16),
            pltpu.VMEM((2 * tokens, exp_ff), BF16),
            pltpu.VMEM((tokens, model), BF16),
            pltpu.VMEM((tokens, model), F32),
            pltpu.SemaphoreType.DMA((48,)),
            pltpu.SemaphoreType.DMA((28,)),
            pltpu.SemaphoreType.DMA((28,)),
        ]
        result = pl.pallas_call(
            functools.partial(kernel, group),
            out_shape=jax.ShapeDtypeStruct((tokens, model), BF16),
            in_specs=[pl.BlockSpec(memory_space=pl.ANY)] * len(args),
            out_specs=pl.BlockSpec(memory_space=pl.ANY),
            scratch_shapes=scratch,
            compiler_params=pltpu.CompilerParams(collective_id=0, has_side_effects=True, vmem_limit_bytes=67043328),
        )(*args)
        return result.reshape(n_seqs, seq_len, model)

    return jax.shard_map(per_device, mesh=mesh, in_specs=(row_spec, row_spec, row_spec, vec_spec, mat_spec, mat_spec, mat_spec, cube_spec, vec_spec, mat_spec, mat_spec, mat_spec, vec_spec, mat_spec, expert_spec, expert_spec, expert_spec), out_specs=row_spec, check_vma=False)
```

```python
import functools

import jax
import jax.numpy as jnp
import numpy as np
from jax import lax
from jax.experimental import pallas as pl
from jax.experimental.pallas import tpu as pltpu
from jax.sharding import PartitionSpec as P

RMS_EPS = 1e-6
ROPE_BASE = 10000.0
MESH = pl.DeviceIdType.MESH
F32, BF16 = jnp.float32, jnp.bfloat16
LANES = 128
FF_BLOCK = 512
COL = 256
N_P = 2
N_O = 4


def rms_rows(row_vals, norm_scale):
    as_float = row_vals.astype(F32)
    inv_rms = lax.rsqrt(jnp.mean(as_float * as_float, axis=-1, keepdims=True) + RMS_EPS)
    return (as_float * inv_rms * norm_scale).astype(BF16)


def silu(z):
    return z / (1.0 + jnp.exp(-z))


def dot(a, b):
    return jnp.dot(a, b, preferred_element_type=F32)


def rope_tables(seq_len, head_dim):
    half = head_dim // 2
    lane = np.arange(LANES)
    freq = ROPE_BASE ** (-2.0 * (lane % half) / head_dim)
    angle = np.arange(seq_len)[:, None] * freq[None, :]
    sign = np.where(lane % head_dim < half, -1.0, 1.0)
    return np.cos(angle).astype(np.float32), (np.sin(angle) * sign[None, :]).astype(np.float32)


def kernel(group, hidden, ids, attn_norm, w_query, w_key, w_value, w_out, ffn_norm, ffn_gate, ffn_up, ffn_down,
           moe_norm, w_router, exp_gate, exp_up, exp_down, cos_t, sin_t, out,
           v_hid, v_ids, v_an, v_wq, v_wk, v_wv, v_wo, v_fn, v_fg, v_fu, v_fd, v_mn, v_wr, v_eg, v_eu, v_ed, v_cos, v_sin,
           v_out, x_buf, g_buf, p_buf, pr_buf, tb, rb, qf, kf, vf, ctx, hb, gate_b, att, ffn_acc,
           w_sem, s_sem, r_sem):
    tokens, model = v_hid.shape
    half, quarter = tokens // 2, tokens // 4
    n_local = v_eg.shape[0]
    exp_ff = v_eg.shape[2]
    ff_dim = v_fg.shape[1]
    n_experts = v_wr.shape[0]
    me = lax.axis_index('ep')
    partner = me + 1 - 2 * lax.rem(me, 2)
    right = lax.rem(me + 2, group)
    left = lax.rem(me + group - 2, group)

    loads = {}

    def load(name, src, dst):
        loads[name] = pltpu.make_async_copy(src, dst, w_sem.at[len(loads)])
        loads[name].start()

    def ready(*names):
        for name in names:
            loads[name].wait()

    copies = {}

    def remote(name, src, dst, device):
        k = len(copies)
        copies[name] = pltpu.make_async_remote_copy(
            src_ref=src, dst_ref=dst, send_sem=s_sem.at[k], recv_sem=r_sem.at[k],
            device_id={'ep': device}, device_id_type=MESH)

    def send(*names):
        for name in names:
            copies[name].start()

    def recv(*names):
        for name in names:
            copies[name].wait_recv()

    lo, hi, al, ot = pl.ds(0, half), pl.ds(half, half), pl.ds(0, tokens), pl.ds(tokens, tokens)
    q0, q1, q2, q3 = (pl.ds(i * quarter, quarter) for i in range(4))
    p_cols = [pl.ds(n * model // N_P, model // N_P) for n in range(N_P)]
    o_cols = [pl.ds(n * model // N_O, model // N_O) for n in range(N_O)]
    for name, c_src, rows, c_dst, device in (
            ('a1a', 0, q0, 1, right), ('a1b', 0, q1, 1, right), ('a2a', 0, q2, 1, left), ('a2b', 0, q3, 1, left),
            ('a3a', 0, q2, 2, right), ('a3b', 0, q3, 2, right), ('a4a', 0, q0, 2, left), ('a4b', 0, q1, 2, left),
            ('f1a', 1, q0, 3, right), ('f1b', 1, q1, 3, right), ('f2a', 1, q2, 3, left), ('f2b', 1, q3, 3, left)):
        remote(name, x_buf.at[c_src, rows], x_buf.at[c_dst, rows], device)
    for c in range(4):
        remote(f'd{c}', x_buf.at[c, al], x_buf.at[c, ot], partner)
    remote('g1', g_buf.at[0, 0], g_buf.at[1, 0], right)
    remote('g2', g_buf.at[0, 0], g_buf.at[2, 0], left)
    remote('g3', g_buf.at[1, 0], g_buf.at[3, 0], right)
    for c in range(4):
        remote(f'gd{c}', g_buf.at[c, 0], g_buf.at[c, 1], partner)
    for n, cols in enumerate(p_cols):
        for c in range(4):
            remote(f'p{c}_{n}', p_buf.at[c, ot, cols], pr_buf.at[c, :, cols], partner)
        remote(f'i1_{n}', p_buf.at[1, hi, cols], rb.at[1, hi, cols], right)
        remote(f'i2_{n}', p_buf.at[1, lo, cols], rb.at[0, lo, cols], left)
    for n, cols in enumerate(o_cols):
        remote(f'o1_{n}', p_buf.at[3, lo, cols], tb.at[lo, cols], right)
        remote(f'o2_{n}', p_buf.at[3, hi, cols], tb.at[hi, cols], left)
        remote(f'w1_{n}', p_buf.at[2, lo, cols], rb.at[1, lo, cols], right)
        remote(f'w2_{n}', p_buf.at[2, hi, cols], rb.at[0, hi, cols], left)

    load('hid', hidden, v_hid)
    load('mn', moe_norm, v_mn)
    load('wr', w_router, v_wr)
    load('ids', ids, v_ids)
    load('an', attn_norm, v_an)
    load('wq', w_query, v_wq)
    load('wk', w_key, v_wk)
    load('wv', w_value, v_wv)
    load('cos', cos_t, v_cos)
    load('sin', sin_t, v_sin)

    barrier = pltpu.get_barrier_semaphore()
    for peer in (partner, left, right):
        pl.semaphore_signal(barrier, inc=1, device_id={'ep': peer}, device_id_type=MESH)

    load('wo', w_out, v_wo)
    for e in range(n_local):
        load(f'eg{e}', exp_gate.at[e], v_eg.at[e])
        load(f'eu{e}', exp_up.at[e], v_eu.at[e])
    for e in range(n_local):
        load(f'ed{e}', exp_down.at[e], v_ed.at[e])
    load('fn', ffn_norm, v_fn)

    def norm_row(ref):
        scale = ref[...].astype(F32)
        return jnp.concatenate([scale[r:r + 1] for r in range(scale.shape[0])], axis=1)

    ready('hid', 'mn')
    x_buf[0, :tokens] = rms_rows(v_hid[...], norm_row(v_mn))
    pl.semaphore_wait(barrier, 3)
    send('a1a', 'a2a', 'a1b', 'a2b', 'd0')

    ready('wr', 'ids')
    logits = lax.dot_general(v_wr[...], x_buf[0, :tokens], (((1,), (1,)), ((), ())), preferred_element_type=F32)
    expert_row = lax.broadcasted_iota(jnp.int32, logits.shape, 0)
    id_vals = v_ids[...]
    mask = expert_row == id_vals[0:1]
    for j in range(1, id_vals.shape[0]):
        mask = jnp.logical_or(mask, expert_row == id_vals[j:j + 1])
    top = jnp.max(jnp.where(mask, logits, -jnp.inf), axis=0, keepdims=True)
    powers = jnp.where(mask, jnp.exp(logits - top), 0.0)
    g_buf[0, 0] = powers / jnp.sum(powers, axis=0, keepdims=True)
    send('g1', 'g2', 'gd0', 'a3a', 'a4a')

    ready('an', 'wq', 'wk', 'wv', 'cos', 'sin')
    normed = rms_rows(v_hid[...], norm_row(v_an))
    qf[...] = dot(normed, v_wq[...])
    kf[...] = dot(normed, v_wk[...])
    vf[...] = dot(normed, v_wv[...])

    lane = lax.broadcasted_iota(jnp.int32, (tokens, LANES), 1)
    low_half = lax.rem(lane, 64) < 32
    head0 = lane < 64
    row = lax.rem(lax.broadcasted_iota(jnp.int32, (2 * tokens, tokens), 0), tokens)
    causal = row >= lax.broadcasted_iota(jnp.int32, (2 * tokens, tokens), 1)

    def rope(x):
        swapped = jnp.where(low_half, pltpu.roll(x, LANES - 32, 1), pltpu.roll(x, 32, 1))
        return x * v_cos[...] + swapped * v_sin[...]

    def attend(t):
        kt = rope(kf[:, t * LANES:(t + 1) * LANES])
        vt = vf[:, t * LANES:(t + 1) * LANES]
        kt_r, vt_r = pltpu.roll(kt, 64, 1), pltpu.roll(vt, 64, 1)
        for s in range(2):
            g = 2 * t + s
            k2 = (jnp.where(head0, kt, kt_r) if s == 0 else jnp.where(head0, kt_r, kt)).astype(BF16)
            v2 = (jnp.where(head0, vt, vt_r) if s == 0 else jnp.where(head0, vt_r, vt)).astype(BF16)
            q = rope(qf[:, g * LANES:(g + 1) * LANES])
            q2 = jnp.concatenate([jnp.where(head0, q, 0.0), jnp.where(head0, 0.0, q)], axis=0).astype(BF16)
            scores = lax.dot_general(q2, k2, (((1,), (1,)), ((), ())), preferred_element_type=F32) * 64 ** -0.5
            scores = jnp.where(causal, scores, -jnp.inf)
            prob = jnp.exp(scores - jnp.max(scores, axis=-1, keepdims=True))
            prob = (prob / jnp.sum(prob, axis=-1, keepdims=True)).astype(BF16)
            both = dot(prob, v2)
            ctx[:, g * LANES:(g + 1) * LANES] = jnp.where(head0, both[:tokens], both[tokens:]).astype(BF16)

    e_lane = lax.broadcasted_iota(jnp.int32, (tokens, n_experts), 1) - me * n_local
    t_lane = lax.broadcasted_iota(jnp.int32, (n_experts, tokens), 1) < half

    def set_gates(c, par):
        if c == 0:
            gt = g_buf[0, par]
        elif c == 3:
            gt = g_buf[3, par]
        elif c == 1:
            gt = jnp.where(t_lane, g_buf[1, par], g_buf[2, par])
        else:
            gt = jnp.where(t_lane, g_buf[2, par], g_buf[1, par])
        gates_c = gt.T
        for e in range(n_local):
            gate = jnp.sum(jnp.where(e_lane == e, gates_c, 0.0), axis=-1, keepdims=True)
            gate_b[e, par * tokens:(par + 1) * tokens] = jnp.broadcast_to(gate, (tokens, LANES))

    def act(c, rows, e):
        x = x_buf[c, rows]
        used = gate_b[e, rows] > 0.0
        used = jnp.concatenate([used.astype(F32)] * (COL // LANES), axis=1) > 0.0
        for n in range(exp_ff // COL):
            cols = slice(n * COL, (n + 1) * COL)
            z = silu(dot(x, v_eg[e, :, cols])) * dot(x, v_eu[e, :, cols])
            hb[rows, e * exp_ff + n * COL:e * exp_ff + (n + 1) * COL] = jnp.where(used, z, 0.0).astype(BF16)

    def down(c):
        for n in range(model // COL):
            cols = slice(n * COL, (n + 1) * COL)
            for e in range(n_local):
                y = dot(hb[:, e * exp_ff:(e + 1) * exp_ff], v_ed[e, :, cols]).astype(BF16).astype(F32)
                y = y * jnp.concatenate([gate_b[e]] * (COL // LANES), axis=1)
                p_buf[c, :, cols] = y if e == 0 else p_buf[c, :, cols] + y
            if (n + 1) * COL % (model // N_P) == 0:
                send(f'p{c}_{((n + 1) * COL) // (model // N_P) - 1}')

    def add_partner(c, n):
        recv(f'p{c}_{n}')
        cols = slice(n * model // N_P, (n + 1) * model // N_P)
        p_buf[c, :tokens, cols] = p_buf[c, :tokens, cols] + pr_buf[c, :, cols]

    def send_near():
        for n in range(N_P):
            add_partner(1, n)
            send(f'i1_{n}', f'i2_{n}')

    def send_far():
        for n in range(N_P):
            add_partner(3, n)
            for k in range(n * N_O // N_P, (n + 1) * N_O // N_P):
                send(f'o1_{k}', f'o2_{k}')

    def pass_on(n):
        cols = slice(n * model // N_O, (n + 1) * model // N_O)
        recv(f'o1_{n}')
        p_buf[2, :half, cols] = p_buf[2, :half, cols] + tb[:half, cols]
        send(f'w1_{n}')
        recv(f'o2_{n}')
        p_buf[2, half:tokens, cols] = p_buf[2, half:tokens, cols] + tb[half:, cols]
        send(f'w2_{n}')

    def ffn_block(b, x):
        act_cols = slice(b * FF_BLOCK, (b + 1) * FF_BLOCK)
        for n in range(FF_BLOCK // COL):
            cols = slice(b * FF_BLOCK + n * COL, b * FF_BLOCK + (n + 1) * COL)
            z = silu(dot(x, v_fg[:, cols])) * dot(x, v_fu[:, cols])
            hb[:tokens, n * COL:(n + 1) * COL] = z.astype(BF16)
        h = hb[:tokens, :FF_BLOCK]
        for n in range(model // COL):
            cols = slice(n * COL, (n + 1) * COL)
            y = dot(h, v_fd[act_cols, cols])
            ffn_acc[:, cols] = y + (att[:, cols].astype(F32) if b == 0 else ffn_acc[:, cols])

    same, other, both = slice(0, tokens), slice(tokens, 2 * tokens), slice(0, 2 * tokens)

    attend(0)
    attend(1)
    attend(2)
    recv('a1a', 'a2a')
    send('f1a', 'f2a')
    attend(3)
    ready('wo', 'fn')
    att[...] = (v_hid[...].astype(F32) + dot(ctx[...], v_wo[...])).astype(BF16)
    recv('a1b', 'a2b')
    send('f1b', 'f2b', 'd1', 'a3b', 'a4b')
    recv('g1', 'g2')
    send('g3', 'gd1', 'gd2')

    n_blk = ff_dim // 1024
    for b in range(n_blk):
        cols = pl.ds(b * 1024, 1024)
        load(f'fg{b}', ffn_gate.at[:, cols], v_fg.at[:, cols])
        load(f'fu{b}', ffn_up.at[:, cols], v_fu.at[:, cols])
        load(f'fd{b}', ffn_down.at[cols], v_fd.at[cols])

    set_gates(1, 0)
    for e in range(n_local):
        ready(f'eg{e}', f'eu{e}')
        act(1, same, e)
    recv('gd1', 'gd2', 'd1')
    set_gates(1, 1)
    for e in range(n_local):
        act(1, other, e)
    for e in range(n_local):
        ready(f'ed{e}')
    down(1)
    recv('f1a', 'f2a', 'f1b', 'f2b')
    send('d3')
    recv('g3')
    send('gd3')
    set_gates(3, 0)
    act(3, same, 0)
    send_near()
    for e in range(1, n_local):
        act(3, same, e)
    recv('gd3', 'd3')
    set_gates(3, 1)
    for e in range(n_local):
        act(3, other, e)
    recv('a3a', 'a3b', 'a4a', 'a4b')
    send('d2')
    down(3)
    set_gates(2, 0)
    for e in range(n_local):
        act(2, same, e)
    send_far()
    recv('d2')
    set_gates(2, 1)
    for e in range(n_local):
        act(2, other, e)
    down(2)
    recv('d0', 'gd0')
    set_gates(0, 0)
    set_gates(0, 1)
    act(0, both, 0)
    act(0, both, 1)
    for n in range(N_P):
        add_partner(2, n)
    act(0, both, 2)
    act(0, both, 3)
    pass_on(0)
    down(0)
    pass_on(1)

    normed_ffn = rms_rows(att[...], norm_row(v_fn))
    n_ffn = ff_dim // FF_BLOCK
    for b in range(n_ffn):
        if (b * FF_BLOCK) % 1024 == 0:
            i = b * FF_BLOCK // 1024
            ready(f'fg{i}', f'fu{i}', f'fd{i}')
        ffn_block(b, normed_ffn)
        if b == 2:
            pass_on(2)
        if b == 5:
            pass_on(3)
    for n in range(N_P):
        add_partner(0, n)
    ffn_acc[...] = ffn_acc[...] + p_buf[0, :tokens]
    for n in range(N_P):
        recv(f'i1_{n}', f'i2_{n}')
    ffn_acc[:half] = ffn_acc[:half] + rb[0, :half]
    ffn_acc[half:] = ffn_acc[half:] + rb[1, half:]
    stores = []
    for n in range(N_O):
        recv(f'w1_{n}', f'w2_{n}')
        cols = slice(n * model // N_O, (n + 1) * model // N_O)
        v_out[:half, cols] = (ffn_acc[:half, cols] + rb[1, :half, cols]).astype(BF16)
        v_out[half:, cols] = (ffn_acc[half:, cols] + rb[0, half:, cols]).astype(BF16)
        stores.append(pltpu.make_async_copy(v_out.at[:, o_cols[n]], out.at[:, o_cols[n]], w_sem.at[len(loads) + n]))
        stores[-1].start()
    for copy in copies.values():
        copy.wait_send()
    for copy in stores:
        copy.wait()


def solution(mesh):
    group = mesh.shape['ep']
    row_spec = P(('dp', 'ep'), None, None)
    vec_spec = P(None)
    mat_spec = P(None, None)
    cube_spec = P(None, None, None)
    expert_spec = P('ep', None, None)

    def per_device(hidden, expert_ids, slot_ids, attn_norm, w_query, w_key, w_value, w_out, ffn_norm, ffn_gate, ffn_up, ffn_down, moe_norm, w_router, exp_gate, exp_up, exp_down):
        n_seqs, seq_len, model = hidden.shape
        tokens = n_seqs * seq_len
        n_heads, head_dim = w_out.shape[0], w_out.shape[1]
        top_k = expert_ids.shape[-1]
        n_local, _, exp_ff = exp_gate.shape
        n_experts = w_router.shape[1]
        kv_dim = w_key.shape[1]
        assert n_seqs == 1 and group == 8 and head_dim == 64
        cos_t, sin_t = rope_tables(seq_len, head_dim)
        args = (hidden.reshape(tokens, model), expert_ids.reshape(tokens, top_k).T, attn_norm.reshape(-1, LANES),
                w_query, w_key, w_value, w_out.reshape(n_heads * head_dim, model), ffn_norm.reshape(-1, LANES),
                ffn_gate, ffn_up, ffn_down, moe_norm.reshape(-1, LANES), w_router.T, exp_gate, exp_up, exp_down,
                jnp.asarray(cos_t), jnp.asarray(sin_t))
        vmem = [pltpu.VMEM(a.shape, a.dtype) for a in args]
        scratch = vmem + [
            pltpu.VMEM((tokens, model), BF16),
            pltpu.VMEM((4, 2 * tokens, model), BF16),
            pltpu.VMEM((4, 2, n_experts, tokens), F32),
            pltpu.VMEM((4, 2 * tokens, model), F32),
            pltpu.VMEM((4, tokens, model), F32),
            pltpu.VMEM((tokens, model), F32),
            pltpu.VMEM((2, tokens, model), F32),
            pltpu.VMEM((tokens, n_heads * head_dim), F32),
            pltpu.VMEM((tokens, kv_dim), F32),
            pltpu.VMEM((tokens, kv_dim), F32),
            pltpu.VMEM((tokens, n_heads * head_dim), BF16),
            pltpu.VMEM((2 * tokens, n_local * exp_ff), BF16),
            pltpu.VMEM((n_local, 2 * tokens, LANES), F32),
            pltpu.VMEM((tokens, model), BF16),
            pltpu.VMEM((tokens, model), F32),
            pltpu.SemaphoreType.DMA((48,)),
            pltpu.SemaphoreType.DMA((56,)),
            pltpu.SemaphoreType.DMA((56,)),
        ]
        result = pl.pallas_call(
            functools.partial(kernel, group),
            out_shape=jax.ShapeDtypeStruct((tokens, model), BF16),
            in_specs=[pl.BlockSpec(memory_space=pl.ANY)] * len(args),
            out_specs=pl.BlockSpec(memory_space=pl.ANY),
            scratch_shapes=scratch,
            compiler_params=pltpu.CompilerParams(collective_id=0, has_side_effects=True, vmem_limit_bytes=67043328),
        )(*args)
        return result.reshape(n_seqs, seq_len, model)

    return jax.shard_map(per_device, mesh=mesh, in_specs=(row_spec, row_spec, row_spec, vec_spec, mat_spec, mat_spec, mat_spec, cube_spec, vec_spec, mat_spec, mat_spec, mat_spec, vec_spec, mat_spec, expert_spec, expert_spec, expert_spec), out_specs=row_spec, check_vma=False)
```

```python
import functools

import jax
import jax.numpy as jnp
import numpy as np
from jax import lax
from jax.experimental import pallas as pl
from jax.experimental.pallas import tpu as pltpu
from jax.sharding import PartitionSpec as P

RMS_EPS = 1e-6
ROPE_BASE = 10000.0
MESH = pl.DeviceIdType.MESH
F32, BF16 = jnp.float32, jnp.bfloat16
LANES = 128
FF_BLOCK = 512
COL = 256
N_P = 4
VMEM_BYTES = 60 * 1024 * 1024


def rms_rows(row_vals, norm_scale):
    as_float = row_vals.astype(F32)
    inv_rms = lax.rsqrt(jnp.mean(as_float * as_float, axis=-1, keepdims=True) + RMS_EPS)
    return (as_float * inv_rms * norm_scale).astype(BF16)


def silu(z):
    return z / (1.0 + jnp.exp(-z))


def dot(a, b):
    return jnp.dot(a, b, preferred_element_type=F32)


def rope_tables(seq_len, head_dim):
    half = head_dim // 2
    lane = np.arange(LANES)
    freq = ROPE_BASE ** (-2.0 * (lane % half) / head_dim)
    angle = np.arange(seq_len)[:, None] * freq[None, :]
    sign = np.where(lane % head_dim < half, -1.0, 1.0)
    return np.cos(angle).astype(np.float32), (np.sin(angle) * sign[None, :]).astype(np.float32)


def kernel(group, hidden, ids, attn_norm, w_query, w_key, w_value, w_out, ffn_norm, ffn_gate, ffn_up, ffn_down,
           moe_norm, w_router, exp_gate, exp_up, exp_down, cos_t, sin_t, total, far,
           v_hid, v_ids, v_an, v_wq, v_wk, v_wv, v_wo, v_fn, v_fg, v_fu, v_fd, v_mn, v_wr, v_eg, v_eu, v_ed, v_cos, v_sin,
           x_buf, g_buf, p_buf, pr_buf, tb, near, qf, kf, vf, ctx, hb, gate_b, att, ffn_acc,
           w_sem, s_sem, r_sem):
    tokens, model = v_hid.shape
    half, quarter = tokens // 2, tokens // 4
    n_local = v_eg.shape[0]
    exp_ff = v_eg.shape[2]
    ff_dim = v_fg.shape[1]
    n_experts = v_wr.shape[0]
    me = lax.axis_index('ep')
    partner = me + 1 - 2 * lax.rem(me, 2)
    right = lax.rem(me + 2, group)
    left = lax.rem(me + group - 2, group)

    loads = {}

    def load(name, src, dst):
        loads[name] = pltpu.make_async_copy(src, dst, w_sem.at[len(loads)])
        loads[name].start()

    def ready(*names):
        for name in names:
            loads[name].wait()

    copies = {}

    def remote(name, src, dst, device):
        k = len(copies)
        copies[name] = pltpu.make_async_remote_copy(
            src_ref=src, dst_ref=dst, send_sem=s_sem.at[k], recv_sem=r_sem.at[k],
            device_id={'ep': device}, device_id_type=MESH)

    def send(*names):
        for name in names:
            copies[name].start()

    def recv(*names):
        for name in names:
            copies[name].wait_recv()

    lo, hi, al, ot = pl.ds(0, half), pl.ds(half, half), pl.ds(0, tokens), pl.ds(tokens, tokens)
    q0, q1, q2, q3 = (pl.ds(i * quarter, quarter) for i in range(4))
    p_cols = [pl.ds(n * model // N_P, model // N_P) for n in range(N_P)]
    for name, c_src, rows, c_dst, device in (
            ('a1a', 0, q0, 1, right), ('a1b', 0, q1, 1, right), ('a2a', 0, q2, 1, left), ('a2b', 0, q3, 1, left),
            ('a3a', 0, q2, 2, right), ('a3b', 0, q3, 2, right), ('a4a', 0, q0, 2, left), ('a4b', 0, q1, 2, left),
            ('f1a', 1, q0, 3, right), ('f1b', 1, q1, 3, right), ('f2a', 1, q2, 3, left), ('f2b', 1, q3, 3, left)):
        remote(name, x_buf.at[c_src, rows], x_buf.at[c_dst, rows], device)
    for c in range(4):
        remote(f'd{c}', x_buf.at[c, al], x_buf.at[c, ot], partner)
    remote('g1', g_buf.at[0, 0], g_buf.at[1, 0], right)
    remote('g2', g_buf.at[0, 0], g_buf.at[2, 0], left)
    remote('g3', g_buf.at[1, 0], g_buf.at[3, 0], right)
    for c in range(4):
        remote(f'gd{c}', g_buf.at[c, 0], g_buf.at[c, 1], partner)
    for n, cols in enumerate(p_cols):
        for c in range(4):
            remote(f'p{c}_{n}', p_buf.at[c, ot, cols], pr_buf.at[c, :, cols], partner)
        remote(f'i1_{n}', p_buf.at[1, hi, cols], near.at[hi, cols], right)
        remote(f'i2_{n}', p_buf.at[1, lo, cols], near.at[lo, cols], left)
        remote(f'o1_{n}', p_buf.at[3, lo, cols], tb.at[lo, cols], right)
        remote(f'o2_{n}', p_buf.at[3, hi, cols], tb.at[hi, cols], left)
        remote(f'w1_{n}', p_buf.at[2, lo, cols], far.at[lo, cols], right)
        remote(f'w2_{n}', p_buf.at[2, hi, cols], far.at[hi, cols], left)

    load('hid', hidden, v_hid)
    load('mn', moe_norm, v_mn)
    load('wr', w_router, v_wr)
    load('ids', ids, v_ids)
    load('an', attn_norm, v_an)
    load('wq', w_query, v_wq)
    load('wk', w_key, v_wk)
    load('wv', w_value, v_wv)
    load('fn', ffn_norm, v_fn)
    load('cos', cos_t, v_cos)
    load('sin', sin_t, v_sin)

    barrier = pltpu.get_barrier_semaphore()
    for peer in (partner, left, right):
        pl.semaphore_signal(barrier, inc=1, device_id={'ep': peer}, device_id_type=MESH)

    load('wo', w_out, v_wo)
    for e in range(n_local):
        load(f'eg{e}', exp_gate.at[e], v_eg.at[e])
        load(f'eu{e}', exp_up.at[e], v_eu.at[e])
    for e in range(n_local):
        load(f'ed{e}', exp_down.at[e], v_ed.at[e])

    def norm_row(ref):
        scale = ref[...].astype(F32)
        return jnp.concatenate([scale[r:r + 1] for r in range(scale.shape[0])], axis=1)

    ready('hid', 'mn')
    x_buf[0, :tokens] = rms_rows(v_hid[...], norm_row(v_mn))
    pl.semaphore_wait(barrier, 3)
    send('a1a', 'a2a', 'a1b', 'a2b', 'd0')

    ready('wr', 'ids')
    logits = lax.dot_general(v_wr[...], x_buf[0, :tokens], (((1,), (1,)), ((), ())), preferred_element_type=F32)
    expert_row = lax.broadcasted_iota(jnp.int32, logits.shape, 0)
    id_vals = v_ids[...]
    mask = expert_row == id_vals[0:1]
    for j in range(1, id_vals.shape[0]):
        mask = jnp.logical_or(mask, expert_row == id_vals[j:j + 1])
    top = jnp.max(jnp.where(mask, logits, -jnp.inf), axis=0, keepdims=True)
    powers = jnp.where(mask, jnp.exp(logits - top), 0.0)
    g_buf[0, 0] = powers / jnp.sum(powers, axis=0, keepdims=True)
    send('g1', 'g2', 'gd0', 'a3a', 'a4a')

    ready('an', 'wq', 'wk', 'wv', 'cos', 'sin')
    normed = rms_rows(v_hid[...], norm_row(v_an))
    qf[...] = dot(normed, v_wq[...])
    kf[...] = dot(normed, v_wk[...])
    vf[...] = dot(normed, v_wv[...])

    lane = lax.broadcasted_iota(jnp.int32, (tokens, LANES), 1)
    low_half = lax.rem(lane, 64) < 32
    head0 = lane < 64
    row = lax.rem(lax.broadcasted_iota(jnp.int32, (2 * tokens, tokens), 0), tokens)
    causal = row >= lax.broadcasted_iota(jnp.int32, (2 * tokens, tokens), 1)

    def rope(x):
        swapped = jnp.where(low_half, pltpu.roll(x, LANES - 32, 1), pltpu.roll(x, 32, 1))
        return x * v_cos[...] + swapped * v_sin[...]

    def attend(t):
        kt = rope(kf[:, t * LANES:(t + 1) * LANES])
        vt = vf[:, t * LANES:(t + 1) * LANES]
        kt_r, vt_r = pltpu.roll(kt, 64, 1), pltpu.roll(vt, 64, 1)
        for s in range(2):
            g = 2 * t + s
            k2 = (jnp.where(head0, kt, kt_r) if s == 0 else jnp.where(head0, kt_r, kt)).astype(BF16)
            v2 = (jnp.where(head0, vt, vt_r) if s == 0 else jnp.where(head0, vt_r, vt)).astype(BF16)
            q = rope(qf[:, g * LANES:(g + 1) * LANES])
            q2 = jnp.concatenate([jnp.where(head0, q, 0.0), jnp.where(head0, 0.0, q)], axis=0).astype(BF16)
            scores = lax.dot_general(q2, k2, (((1,), (1,)), ((), ())), preferred_element_type=F32) * 64 ** -0.5
            scores = jnp.where(causal, scores, -jnp.inf)
            prob = jnp.exp(scores - jnp.max(scores, axis=-1, keepdims=True))
            prob = (prob / jnp.sum(prob, axis=-1, keepdims=True)).astype(BF16)
            both = dot(prob, v2)
            ctx[:, g * LANES:(g + 1) * LANES] = jnp.where(head0, both[:tokens], both[tokens:]).astype(BF16)

    e_lane = lax.broadcasted_iota(jnp.int32, (tokens, n_experts), 1) - me * n_local
    t_lane = lax.broadcasted_iota(jnp.int32, (n_experts, tokens), 1) < half

    def set_gates(c, par):
        if c == 0:
            gt = g_buf[0, par]
        elif c == 3:
            gt = g_buf[3, par]
        elif c == 1:
            gt = jnp.where(t_lane, g_buf[1, par], g_buf[2, par])
        else:
            gt = jnp.where(t_lane, g_buf[2, par], g_buf[1, par])
        gates_c = gt.T
        for e in range(n_local):
            gate = jnp.sum(jnp.where(e_lane == e, gates_c, 0.0), axis=-1, keepdims=True)
            gate_b[e, par * tokens:(par + 1) * tokens] = jnp.broadcast_to(gate, (tokens, LANES))

    def act(c, rows, e):
        x = x_buf[c, rows]
        used = gate_b[e, rows] > 0.0
        used = jnp.concatenate([used.astype(F32)] * (COL // LANES), axis=1) > 0.0
        for n in range(exp_ff // COL):
            cols = slice(n * COL, (n + 1) * COL)
            z = silu(dot(x, v_eg[e, :, cols])) * dot(x, v_eu[e, :, cols])
            hb[rows, e * exp_ff + n * COL:e * exp_ff + (n + 1) * COL] = jnp.where(used, z, 0.0).astype(BF16)

    def down(c):
        for n in range(model // COL):
            cols = slice(n * COL, (n + 1) * COL)
            for e in range(n_local):
                y = dot(hb[:, e * exp_ff:(e + 1) * exp_ff], v_ed[e, :, cols]).astype(BF16).astype(F32)
                y = y * jnp.concatenate([gate_b[e]] * (COL // LANES), axis=1)
                p_buf[c, :, cols] = y if e == 0 else p_buf[c, :, cols] + y
            if (n + 1) * COL % (model // N_P) == 0:
                send(f'p{c}_{((n + 1) * COL) // (model // N_P) - 1}')

    def add_partner(c, n):
        recv(f'p{c}_{n}')
        cols = slice(n * model // N_P, (n + 1) * model // N_P)
        p_buf[c, :tokens, cols] = p_buf[c, :tokens, cols] + pr_buf[c, :, cols]

    def send_near(n):
        add_partner(1, n)
        send(f'i1_{n}', f'i2_{n}')

    def send_far(n):
        add_partner(3, n)
        send(f'o1_{n}', f'o2_{n}')

    def pass_on(n):
        add_partner(2, n)
        cols = slice(n * model // N_P, (n + 1) * model // N_P)
        recv(f'o1_{n}')
        p_buf[2, :half, cols] = p_buf[2, :half, cols] + tb[:half, cols]
        send(f'w1_{n}')
        recv(f'o2_{n}')
        p_buf[2, half:tokens, cols] = p_buf[2, half:tokens, cols] + tb[half:, cols]
        send(f'w2_{n}')

    def ffn_block(b, x):
        act_cols = slice(b * FF_BLOCK, (b + 1) * FF_BLOCK)
        for n in range(FF_BLOCK // COL):
            cols = slice(b * FF_BLOCK + n * COL, b * FF_BLOCK + (n + 1) * COL)
            z = silu(dot(x, v_fg[:, cols])) * dot(x, v_fu[:, cols])
            hb[:tokens, n * COL:(n + 1) * COL] = z.astype(BF16)
        h = hb[:tokens, :FF_BLOCK]
        for n in range(model // COL):
            cols = slice(n * COL, (n + 1) * COL)
            y = dot(h, v_fd[act_cols, cols])
            ffn_acc[:, cols] = y + (att[:, cols].astype(F32) if b == 0 else ffn_acc[:, cols])

    same, other, both = slice(0, tokens), slice(tokens, 2 * tokens), slice(0, 2 * tokens)

    attend(0)
    attend(1)
    attend(2)
    recv('a1a', 'a2a')
    send('f1a', 'f2a')
    attend(3)
    ready('wo', 'fn')
    att[...] = (v_hid[...].astype(F32) + dot(ctx[...], v_wo[...])).astype(BF16)
    recv('a1b', 'a2b')
    send('f1b', 'f2b', 'd1')
    recv('g1', 'g2')
    send('g3', 'gd1', 'gd2', 'a3b', 'a4b')

    n_blk = ff_dim // 1024
    for b in range(n_blk):
        cols = pl.ds(b * 1024, 1024)
        load(f'fg{b}', ffn_gate.at[:, cols], v_fg.at[:, cols])
        load(f'fu{b}', ffn_up.at[:, cols], v_fu.at[:, cols])
        load(f'fd{b}', ffn_down.at[cols], v_fd.at[cols])

    set_gates(1, 0)
    for e in range(n_local):
        ready(f'eg{e}', f'eu{e}')
        act(1, same, e)
    recv('gd1', 'gd2', 'd1')
    set_gates(1, 1)
    for e in range(n_local):
        act(1, other, e)
    for e in range(n_local):
        ready(f'ed{e}')
    down(1)
    send_near(0)
    recv('f1a', 'f2a', 'f1b', 'f2b')
    send('d3')
    recv('g3')
    send('gd3')
    send_near(1)
    set_gates(3, 0)
    act(3, same, 0)
    send_near(2)
    send_near(3)
    for e in range(1, n_local):
        act(3, same, e)
    recv('gd3', 'd3')
    set_gates(3, 1)
    for e in range(n_local):
        act(3, other, e)
    recv('a3a', 'a3b', 'a4a', 'a4b')
    send('d2')
    down(3)
    set_gates(2, 0)
    act(2, same, 0)
    send_far(0)
    act(2, same, 1)
    send_far(1)
    act(2, same, 2)
    send_far(2)
    act(2, same, 3)
    send_far(3)
    recv('d2')
    set_gates(2, 1)
    for e in range(n_local):
        act(2, other, e)
    down(2)
    recv('d0', 'gd0')
    set_gates(0, 0)
    set_gates(0, 1)
    for e in range(n_local):
        act(0, both, e)
    pass_on(0)
    down(0)
    pass_on(1)

    normed_ffn = rms_rows(att[...], norm_row(v_fn))
    n_ffn = ff_dim // FF_BLOCK
    for b in range(n_ffn):
        if (b * FF_BLOCK) % 1024 == 0:
            i = b * FF_BLOCK // 1024
            ready(f'fg{i}', f'fu{i}', f'fd{i}')
        ffn_block(b, normed_ffn)
        if b in (1, 3):
            pass_on((b + 3) // 2)
    for n in range(N_P):
        add_partner(0, n)
    ffn_acc[...] = ffn_acc[...] + p_buf[0, :tokens]
    for n in range(N_P):
        recv(f'i1_{n}', f'i2_{n}')
    late = tuple(f'w{k}_{n}' for k in (1, 2) for n in range(N_P))
    for name, copy in copies.items():
        if name not in late:
            copy.wait_send()
    total[...] = ffn_acc[...] + near[...]
    for name in late:
        copies[name].wait_recv()
        copies[name].wait_send()


def solution(mesh):
    group = mesh.shape['ep']
    row_spec = P(('dp', 'ep'), None, None)
    vec_spec = P(None)
    mat_spec = P(None, None)
    cube_spec = P(None, None, None)
    expert_spec = P('ep', None, None)

    def per_device(hidden, expert_ids, slot_ids, attn_norm, w_query, w_key, w_value, w_out, ffn_norm, ffn_gate, ffn_up, ffn_down, moe_norm, w_router, exp_gate, exp_up, exp_down):
        n_seqs, seq_len, model = hidden.shape
        tokens = n_seqs * seq_len
        n_heads, head_dim = w_out.shape[0], w_out.shape[1]
        top_k = expert_ids.shape[-1]
        n_local, _, exp_ff = exp_gate.shape
        n_experts = w_router.shape[1]
        kv_dim = w_key.shape[1]
        assert n_seqs == 1 and group == 8 and head_dim == 64
        cos_t, sin_t = rope_tables(seq_len, head_dim)
        args = (hidden.reshape(tokens, model), expert_ids.reshape(tokens, top_k).T, attn_norm.reshape(-1, LANES),
                w_query, w_key, w_value, w_out.reshape(n_heads * head_dim, model), ffn_norm.reshape(-1, LANES),
                ffn_gate, ffn_up, ffn_down, moe_norm.reshape(-1, LANES), w_router.T, exp_gate, exp_up, exp_down,
                jnp.asarray(cos_t), jnp.asarray(sin_t))
        vmem = [pltpu.VMEM(a.shape, a.dtype) for a in args]
        scratch = vmem + [
            pltpu.VMEM((4, 2 * tokens, model), BF16),
            pltpu.VMEM((4, 2, n_experts, tokens), F32),
            pltpu.VMEM((4, 2 * tokens, model), F32),
            pltpu.VMEM((4, tokens, model), F32),
            pltpu.VMEM((tokens, model), F32),
            pltpu.VMEM((tokens, model), F32),
            pltpu.VMEM((tokens, n_heads * head_dim), F32),
            pltpu.VMEM((tokens, kv_dim), F32),
            pltpu.VMEM((tokens, kv_dim), F32),
            pltpu.VMEM((tokens, n_heads * head_dim), BF16),
            pltpu.VMEM((2 * tokens, n_local * exp_ff), BF16),
            pltpu.VMEM((n_local, 2 * tokens, LANES), F32),
            pltpu.VMEM((tokens, model), BF16),
            pltpu.VMEM((tokens, model), F32),
            pltpu.SemaphoreType.DMA((48,)),
            pltpu.SemaphoreType.DMA((64,)),
            pltpu.SemaphoreType.DMA((64,)),
        ]
        total, far = pl.pallas_call(
            functools.partial(kernel, group),
            out_shape=(pltpu.VMEM((tokens, model), F32), pltpu.VMEM((tokens, model), F32)),
            in_specs=[pl.BlockSpec(memory_space=pl.ANY)] * len(args),
            out_specs=(pl.BlockSpec(memory_space=pltpu.VMEM),) * 2,
            scratch_shapes=scratch,
            compiler_params=pltpu.CompilerParams(collective_id=0, has_side_effects=True, vmem_limit_bytes=VMEM_BYTES),
        )(*args)
        return (total + far).astype(BF16).reshape(n_seqs, seq_len, model)

    return jax.shard_map(per_device, mesh=mesh, in_specs=(row_spec, row_spec, row_spec, vec_spec, mat_spec, mat_spec, mat_spec, cube_spec, vec_spec, mat_spec, mat_spec, mat_spec, vec_spec, mat_spec, expert_spec, expert_spec, expert_spec), out_specs=row_spec, check_vma=False)
```

```python
import functools

import jax
import jax.numpy as jnp
import numpy as np
from jax import lax
from jax.experimental import pallas as pl
from jax.experimental.pallas import tpu as pltpu
from jax.sharding import PartitionSpec as P

RMS_EPS = 1e-6
ROPE_BASE = 10000.0
MESH = pl.DeviceIdType.MESH
F32, BF16 = jnp.float32, jnp.bfloat16
LANES = 128
FF_BLOCK = 512
COL = 256
N_P = 2
N_O = 4
VMEM_BYTES = 60 * 1024 * 1024


def rms_rows(row_vals, norm_scale):
    as_float = row_vals.astype(F32)
    inv_rms = lax.rsqrt(jnp.mean(as_float * as_float, axis=-1, keepdims=True) + RMS_EPS)
    return (as_float * inv_rms * norm_scale).astype(BF16)


def silu(z):
    return z / (1.0 + jnp.exp(-z))


def dot(a, b):
    return jnp.dot(a, b, preferred_element_type=F32)


def rope_tables(seq_len, head_dim):
    half = head_dim // 2
    lane = np.arange(LANES)
    freq = ROPE_BASE ** (-2.0 * (lane % half) / head_dim)
    angle = np.arange(seq_len)[:, None] * freq[None, :]
    sign = np.where(lane % head_dim < half, -1.0, 1.0)
    return np.cos(angle).astype(np.float32), (np.sin(angle) * sign[None, :]).astype(np.float32)


def kernel(group, hidden, ids, attn_norm, w_query, w_key, w_value, w_out, ffn_norm, ffn_gate, ffn_up, ffn_down,
           moe_norm, w_router, exp_gate, exp_up, exp_down, cos_t, sin_t, total, far,
           v_hid, v_ids, v_an, v_wq, v_wk, v_wv, v_wo, v_fn, v_fg, v_fu, v_fd, v_mn, v_wr, v_eg, v_eu, v_ed, v_cos, v_sin,
           x_buf, g_buf, p_buf, pr_buf, tb, near, qf, kf, vf, ctx, hb, gate_b, att, ffn_acc,
           w_sem, s_sem, r_sem):
    tokens, model = v_hid.shape
    half, quarter = tokens // 2, tokens // 4
    n_local = v_eg.shape[0]
    exp_ff = v_eg.shape[2]
    ff_dim = v_fg.shape[1]
    n_experts = v_wr.shape[0]
    me = lax.axis_index('ep')
    partner = me + 1 - 2 * lax.rem(me, 2)
    right = lax.rem(me + 2, group)
    left = lax.rem(me + group - 2, group)

    loads = {}

    def load(name, src, dst):
        loads[name] = pltpu.make_async_copy(src, dst, w_sem.at[len(loads)])
        loads[name].start()

    def ready(*names):
        for name in names:
            loads[name].wait()

    copies = {}

    def remote(name, src, dst, device):
        k = len(copies)
        copies[name] = pltpu.make_async_remote_copy(
            src_ref=src, dst_ref=dst, send_sem=s_sem.at[k], recv_sem=r_sem.at[k],
            device_id={'ep': device}, device_id_type=MESH)

    def send(*names):
        for name in names:
            copies[name].start()

    def recv(*names):
        for name in names:
            copies[name].wait_recv()

    lo, hi, al, ot = pl.ds(0, half), pl.ds(half, half), pl.ds(0, tokens), pl.ds(tokens, tokens)
    q0, q1, q2, q3 = (pl.ds(i * quarter, quarter) for i in range(4))
    p_cols = [pl.ds(n * model // N_P, model // N_P) for n in range(N_P)]
    for name, c_src, rows, c_dst, device in (
            ('a1a', 0, q0, 1, right), ('a1b', 0, q1, 1, right), ('a2a', 0, q2, 1, left), ('a2b', 0, q3, 1, left),
            ('a3a', 0, q2, 2, right), ('a3b', 0, q3, 2, right), ('a4a', 0, q0, 2, left), ('a4b', 0, q1, 2, left),
            ('f1a', 1, q0, 3, right), ('f1b', 1, q1, 3, right), ('f2a', 1, q2, 3, left), ('f2b', 1, q3, 3, left)):
        remote(name, x_buf.at[c_src, rows], x_buf.at[c_dst, rows], device)
    for c in range(4):
        remote(f'd{c}', x_buf.at[c, al], x_buf.at[c, ot], partner)
    remote('g1', g_buf.at[0, 0], g_buf.at[1, 0], right)
    remote('g2', g_buf.at[0, 0], g_buf.at[2, 0], left)
    remote('g3', g_buf.at[1, 0], g_buf.at[3, 0], right)
    for c in range(4):
        remote(f'gd{c}', g_buf.at[c, 0], g_buf.at[c, 1], partner)
    for n, cols in enumerate(p_cols):
        for c in range(4):
            remote(f'p{c}_{n}', p_buf.at[c, ot, cols], pr_buf.at[c, :, cols], partner)
        remote(f'i1_{n}', p_buf.at[1, hi, cols], near.at[hi, cols], right)
        remote(f'i2_{n}', p_buf.at[1, lo, cols], near.at[lo, cols], left)
    o_cols = [pl.ds(n * model // N_O, model // N_O) for n in range(N_O)]
    for n, cols in enumerate(o_cols):
        remote(f'o1_{n}', p_buf.at[3, lo, cols], tb.at[lo, cols], right)
        remote(f'o2_{n}', p_buf.at[3, hi, cols], tb.at[hi, cols], left)
        remote(f'w1_{n}', p_buf.at[2, lo, cols], far.at[lo, cols], right)
        remote(f'w2_{n}', p_buf.at[2, hi, cols], far.at[hi, cols], left)

    load('hid', hidden, v_hid)
    load('mn', moe_norm, v_mn)
    load('wr', w_router, v_wr)
    load('ids', ids, v_ids)
    load('an', attn_norm, v_an)
    load('wq', w_query, v_wq)
    load('wk', w_key, v_wk)
    load('wv', w_value, v_wv)
    load('fn', ffn_norm, v_fn)
    load('cos', cos_t, v_cos)
    load('sin', sin_t, v_sin)

    barrier = pltpu.get_barrier_semaphore()
    for peer in (partner, left, right):
        pl.semaphore_signal(barrier, inc=1, device_id={'ep': peer}, device_id_type=MESH)

    load('wo', w_out, v_wo)
    for e in range(n_local):
        load(f'eg{e}', exp_gate.at[e], v_eg.at[e])
        load(f'eu{e}', exp_up.at[e], v_eu.at[e])
    for e in range(n_local):
        load(f'ed{e}', exp_down.at[e], v_ed.at[e])

    def norm_row(ref):
        scale = ref[...].astype(F32)
        return jnp.concatenate([scale[r:r + 1] for r in range(scale.shape[0])], axis=1)

    ready('hid', 'mn')
    x_buf[0, :tokens] = rms_rows(v_hid[...], norm_row(v_mn))
    pl.semaphore_wait(barrier, 3)
    send('a1a', 'a2a', 'a1b', 'a2b', 'd0')

    ready('wr', 'ids')
    logits = lax.dot_general(v_wr[...], x_buf[0, :tokens], (((1,), (1,)), ((), ())), preferred_element_type=F32)
    expert_row = lax.broadcasted_iota(jnp.int32, logits.shape, 0)
    id_vals = v_ids[...]
    mask = expert_row == id_vals[0:1]
    for j in range(1, id_vals.shape[0]):
        mask = jnp.logical_or(mask, expert_row == id_vals[j:j + 1])
    top = jnp.max(jnp.where(mask, logits, -jnp.inf), axis=0, keepdims=True)
    powers = jnp.where(mask, jnp.exp(logits - top), 0.0)
    g_buf[0, 0] = powers / jnp.sum(powers, axis=0, keepdims=True)
    send('g1', 'g2', 'gd0', 'a3a', 'a4a')

    ready('an', 'wq', 'wk', 'wv', 'cos', 'sin')
    normed = rms_rows(v_hid[...], norm_row(v_an))
    qf[...] = dot(normed, v_wq[...])
    kf[...] = dot(normed, v_wk[...])
    vf[...] = dot(normed, v_wv[...])

    lane = lax.broadcasted_iota(jnp.int32, (tokens, LANES), 1)
    low_half = lax.rem(lane, 64) < 32
    head0 = lane < 64
    row = lax.rem(lax.broadcasted_iota(jnp.int32, (2 * tokens, tokens), 0), tokens)
    causal = row >= lax.broadcasted_iota(jnp.int32, (2 * tokens, tokens), 1)

    def rope(x):
        swapped = jnp.where(low_half, pltpu.roll(x, LANES - 32, 1), pltpu.roll(x, 32, 1))
        return x * v_cos[...] + swapped * v_sin[...]

    def attend(t):
        kt = rope(kf[:, t * LANES:(t + 1) * LANES])
        vt = vf[:, t * LANES:(t + 1) * LANES]
        kt_r, vt_r = pltpu.roll(kt, 64, 1), pltpu.roll(vt, 64, 1)
        for s in range(2):
            g = 2 * t + s
            k2 = (jnp.where(head0, kt, kt_r) if s == 0 else jnp.where(head0, kt_r, kt)).astype(BF16)
            v2 = (jnp.where(head0, vt, vt_r) if s == 0 else jnp.where(head0, vt_r, vt)).astype(BF16)
            q = rope(qf[:, g * LANES:(g + 1) * LANES])
            q2 = jnp.concatenate([jnp.where(head0, q, 0.0), jnp.where(head0, 0.0, q)], axis=0).astype(BF16)
            scores = lax.dot_general(q2, k2, (((1,), (1,)), ((), ())), preferred_element_type=F32) * 64 ** -0.5
            scores = jnp.where(causal, scores, -jnp.inf)
            prob = jnp.exp(scores - jnp.max(scores, axis=-1, keepdims=True))
            prob = (prob / jnp.sum(prob, axis=-1, keepdims=True)).astype(BF16)
            both = dot(prob, v2)
            ctx[:, g * LANES:(g + 1) * LANES] = jnp.where(head0, both[:tokens], both[tokens:]).astype(BF16)

    e_lane = lax.broadcasted_iota(jnp.int32, (tokens, n_experts), 1) - me * n_local
    t_lane = lax.broadcasted_iota(jnp.int32, (n_experts, tokens), 1) < half

    def set_gates(c, par):
        if c == 0:
            gt = g_buf[0, par]
        elif c == 3:
            gt = g_buf[3, par]
        elif c == 1:
            gt = jnp.where(t_lane, g_buf[1, par], g_buf[2, par])
        else:
            gt = jnp.where(t_lane, g_buf[2, par], g_buf[1, par])
        gates_c = gt.T
        for e in range(n_local):
            gate = jnp.sum(jnp.where(e_lane == e, gates_c, 0.0), axis=-1, keepdims=True)
            gate_b[int(c == 0), e, par * tokens:(par + 1) * tokens] = jnp.broadcast_to(gate, (tokens, LANES))

    def act(c, rows, e):
        x = x_buf[c, rows]
        used = jnp.concatenate([gate_b[int(c == 0), e, rows]] * (COL // LANES), axis=1) > 0.0
        for n in range(exp_ff // COL):
            cols = slice(n * COL, (n + 1) * COL)
            z = silu(dot(x, v_eg[e, :, cols])) * dot(x, v_eu[e, :, cols])
            hb[int(c == 0), rows, e * exp_ff + n * COL:e * exp_ff + (n + 1) * COL] = jnp.where(used, z, 0.0).astype(BF16)

    def down(c, part):
        for n in range(part * model // N_P // COL, (part + 1) * model // N_P // COL):
            cols = slice(n * COL, (n + 1) * COL)
            for e in range(n_local):
                y = dot(hb[int(c == 0), :, e * exp_ff:(e + 1) * exp_ff], v_ed[e, :, cols]).astype(BF16).astype(F32)
                y = y * jnp.concatenate([gate_b[int(c == 0), e]] * (COL // LANES), axis=1)
                p_buf[c, :, cols] = y if e == 0 else p_buf[c, :, cols] + y
        send(f'p{c}_{part}')

    def add_partner(c, n):
        recv(f'p{c}_{n}')
        cols = slice(n * model // N_P, (n + 1) * model // N_P)
        p_buf[c, :tokens, cols] = p_buf[c, :tokens, cols] + pr_buf[c, :, cols]

    def send_near(n):
        add_partner(1, n)
        send(f'i1_{n}', f'i2_{n}')

    def send_far(n):
        add_partner(3, n)
        send(*(f'o{k}_{m}' for m in range(n * N_O // N_P, (n + 1) * N_O // N_P) for k in (1, 2)))

    def pass_on(n):
        cols = slice(n * model // N_O, (n + 1) * model // N_O)
        recv(f'o1_{n}', f'o2_{n}')
        p_buf[2, :tokens, cols] = p_buf[2, :tokens, cols] + tb[:, cols]
        send(f'w1_{n}', f'w2_{n}')

    def ffn_block(b, x):
        act_cols = slice(b * FF_BLOCK, (b + 1) * FF_BLOCK)
        for n in range(FF_BLOCK // COL):
            cols = slice(b * FF_BLOCK + n * COL, b * FF_BLOCK + (n + 1) * COL)
            z = silu(dot(x, v_fg[:, cols])) * dot(x, v_fu[:, cols])
            hb[0, :tokens, n * COL:(n + 1) * COL] = z.astype(BF16)
        h = hb[0, :tokens, :FF_BLOCK]
        for n in range(model // COL):
            cols = slice(n * COL, (n + 1) * COL)
            y = dot(h, v_fd[act_cols, cols])
            ffn_acc[:, cols] = y + (att[:, cols].astype(F32) if b == 0 else ffn_acc[:, cols])

    same, other, both = slice(0, tokens), slice(tokens, 2 * tokens), slice(0, 2 * tokens)
    attend(0)
    attend(1)
    attend(2)
    recv('a1a', 'a2a')
    send('f1a', 'f2a')
    attend(3)
    ready('wo', 'fn')
    att[...] = (v_hid[...].astype(F32) + dot(ctx[...], v_wo[...])).astype(BF16)
    recv('a1b', 'a2b')
    send('f1b', 'f2b', 'd1')
    recv('g1', 'g2')
    send('g3', 'gd1', 'gd2', 'a3b', 'a4b')

    n_blk = ff_dim // 1024
    for b in range(n_blk):
        cols = pl.ds(b * 1024, 1024)
        load(f'fg{b}', ffn_gate.at[:, cols], v_fg.at[:, cols])
        load(f'fu{b}', ffn_up.at[:, cols], v_fu.at[:, cols])
        load(f'fd{b}', ffn_down.at[cols], v_fd.at[cols])

    for e in range(n_local):
        ready(f'eg{e}', f'eu{e}')
    set_gates(1, 0)
    for e in range(n_local):
        act(1, same, e)
    recv('gd1', 'gd2', 'd1')
    for e in range(n_local):
        ready(f'ed{e}')
    set_gates(1, 1)
    for e in range(n_local):
        act(1, other, e)
    down(1, 0)
    down(1, 1)
    recv('f1a', 'f2a', 'f1b', 'f2b')
    send('d3')
    recv('g3')
    send('gd3')
    recv('d0', 'gd0')
    set_gates(0, 0)
    set_gates(0, 1)
    act(0, both, 0)
    send_near(0)
    act(0, both, 1)
    send_near(1)
    recv('gd3', 'd3')
    set_gates(3, 0)
    set_gates(3, 1)
    for e in range(n_local):
        act(3, both, e)
    recv('a3a', 'a3b', 'a4a', 'a4b')
    send('d2')
    down(3, 0)
    down(3, 1)
    act(0, both, 2)
    send_far(0)
    act(0, both, 3)
    send_far(1)
    recv('d2')
    set_gates(2, 0)
    set_gates(2, 1)
    for e in range(n_local):
        act(2, both, e)
    down(2, 0)
    down(2, 1)
    down(0, 0)
    add_partner(2, 0)
    pass_on(0)
    down(0, 1)
    add_partner(2, 1)
    pass_on(1)
    for b in range(n_blk):
        ready(f'fg{b}', f'fu{b}', f'fd{b}')
    normed_ffn = rms_rows(att[...], norm_row(v_fn))
    n_ffn = ff_dim // FF_BLOCK
    for b in range(n_ffn):
        ffn_block(b, normed_ffn)
        if b == 0:
            pass_on(2)
        if b == 2:
            pass_on(3)
    for n in range(N_P):
        add_partner(0, n)
        recv(f'i1_{n}', f'i2_{n}')
    late = tuple(f'w{k}_{n}' for k in (1, 2) for n in range(N_O))
    for name, copy in copies.items():
        if name not in late:
            copy.wait_send()
    total[...] = ffn_acc[...] + p_buf[0, :tokens] + near[...]
    for name in late:
        copies[name].wait_recv()
        copies[name].wait_send()


def solution(mesh):
    group = mesh.shape['ep']
    row_spec = P(('dp', 'ep'), None, None)
    vec_spec = P(None)
    mat_spec = P(None, None)
    cube_spec = P(None, None, None)
    expert_spec = P('ep', None, None)

    def per_device(hidden, expert_ids, slot_ids, attn_norm, w_query, w_key, w_value, w_out, ffn_norm, ffn_gate, ffn_up, ffn_down, moe_norm, w_router, exp_gate, exp_up, exp_down):
        n_seqs, seq_len, model = hidden.shape
        tokens = n_seqs * seq_len
        n_heads, head_dim = w_out.shape[0], w_out.shape[1]
        top_k = expert_ids.shape[-1]
        n_local, _, exp_ff = exp_gate.shape
        n_experts = w_router.shape[1]
        kv_dim = w_key.shape[1]
        assert n_seqs == 1 and group == 8 and head_dim == 64
        cos_t, sin_t = rope_tables(seq_len, head_dim)
        args = (hidden.reshape(tokens, model), expert_ids.reshape(tokens, top_k).T, attn_norm.reshape(-1, LANES),
                w_query, w_key, w_value, w_out.reshape(n_heads * head_dim, model), ffn_norm.reshape(-1, LANES),
                ffn_gate, ffn_up, ffn_down, moe_norm.reshape(-1, LANES), w_router.T, exp_gate, exp_up, exp_down,
                jnp.asarray(cos_t), jnp.asarray(sin_t))
        vmem = [pltpu.VMEM(a.shape, a.dtype) for a in args]
        scratch = vmem + [
            pltpu.VMEM((4, 2 * tokens, model), BF16),
            pltpu.VMEM((4, 2, n_experts, tokens), F32),
            pltpu.VMEM((4, 2 * tokens, model), F32),
            pltpu.VMEM((4, tokens, model), F32),
            pltpu.VMEM((tokens, model), F32),
            pltpu.VMEM((tokens, model), F32),
            pltpu.VMEM((tokens, n_heads * head_dim), F32),
            pltpu.VMEM((tokens, kv_dim), F32),
            pltpu.VMEM((tokens, kv_dim), F32),
            pltpu.VMEM((tokens, n_heads * head_dim), BF16),
            pltpu.VMEM((2, 2 * tokens, n_local * exp_ff), BF16),
            pltpu.VMEM((2, n_local, 2 * tokens, LANES), F32),
            pltpu.VMEM((tokens, model), BF16),
            pltpu.VMEM((tokens, model), F32),
            pltpu.SemaphoreType.DMA((48,)),
            pltpu.SemaphoreType.DMA((64,)),
            pltpu.SemaphoreType.DMA((64,)),
        ]
        total, far = pl.pallas_call(
            functools.partial(kernel, group),
            out_shape=(pltpu.VMEM((tokens, model), F32), pltpu.VMEM((tokens, model), F32)),
            in_specs=[pl.BlockSpec(memory_space=pl.ANY)] * len(args),
            out_specs=(pl.BlockSpec(memory_space=pltpu.VMEM),) * 2,
            scratch_shapes=scratch,
            compiler_params=pltpu.CompilerParams(collective_id=0, has_side_effects=True, vmem_limit_bytes=VMEM_BYTES),
        )(*args)
        return (total + far).astype(BF16).reshape(n_seqs, seq_len, model)

    return jax.shard_map(per_device, mesh=mesh, in_specs=(row_spec, row_spec, row_spec, vec_spec, mat_spec, mat_spec, mat_spec, cube_spec, vec_spec, mat_spec, mat_spec, mat_spec, vec_spec, mat_spec, expert_spec, expert_spec, expert_spec), out_specs=row_spec, check_vma=False)
```

```python
import functools

import jax
import jax.numpy as jnp
import numpy as np
from jax import lax
from jax.experimental import pallas as pl
from jax.experimental.pallas import tpu as pltpu
from jax.sharding import PartitionSpec as P

RMS_EPS = 1e-6
ROPE_BASE = 10000.0
MESH = pl.DeviceIdType.MESH
F32, BF16 = jnp.float32, jnp.bfloat16
LANES = 128
FF_BLOCK = 512
COL = 256
N_P = 2
VMEM_BYTES = 60 * 1024 * 1024


def rms_rows(row_vals, norm_scale):
    as_float = row_vals.astype(F32)
    inv_rms = lax.rsqrt(jnp.mean(as_float * as_float, axis=-1, keepdims=True) + RMS_EPS)
    return (as_float * inv_rms * norm_scale).astype(BF16)


def silu(z):
    half = 0.5 * z
    return half + half * jnp.tanh(half)


def dot(a, b):
    return jnp.dot(a, b, preferred_element_type=F32)


def rope_tables(seq_len, head_dim):
    half = head_dim // 2
    lane = np.arange(LANES)
    freq = ROPE_BASE ** (-2.0 * (lane % half) / head_dim)
    angle = np.arange(seq_len)[:, None] * freq[None, :]
    sign = np.where(lane % head_dim < half, -1.0, 1.0)
    return np.cos(angle).astype(np.float32), (np.sin(angle) * sign[None, :]).astype(np.float32)


def kernel(group, hidden, ids, attn_norm, w_query, w_key, w_value, w_out, ffn_norm, ffn_gate, ffn_up, ffn_down,
           moe_norm, w_router, exp_gate, exp_up, exp_down, cos_t, sin_t, total, far,
           v_hid, v_ids, v_an, v_wq, v_wk, v_wv, v_wo, v_fn, v_fg, v_fu, v_fd, v_mn, v_wr, v_eg, v_eu, v_ed, v_cos, v_sin,
           x_buf, g_buf, p_buf, pr_buf, tb, near, qf, kf, vf, ctx, hb, gate_b, att, ffn_acc,
           w_sem, s_sem, r_sem):
    tokens, model = v_hid.shape
    half, quarter = tokens // 2, tokens // 4
    n_local = v_eg.shape[0]
    exp_ff = v_eg.shape[2]
    ff_dim = v_fg.shape[1]
    n_experts = v_wr.shape[0]
    me = lax.axis_index('ep')
    partner = me + 1 - 2 * lax.rem(me, 2)
    right = lax.rem(me + 2, group)
    left = lax.rem(me + group - 2, group)

    loads = {}

    def load(name, src, dst):
        loads[name] = pltpu.make_async_copy(src, dst, w_sem.at[len(loads)])
        loads[name].start()

    def ready(*names):
        for name in names:
            loads[name].wait()

    copies = {}

    def remote(name, src, dst, device):
        k = len(copies)
        copies[name] = pltpu.make_async_remote_copy(
            src_ref=src, dst_ref=dst, send_sem=s_sem.at[k], recv_sem=r_sem.at[k],
            device_id={'ep': device}, device_id_type=MESH)

    def send(*names):
        for name in names:
            copies[name].start()

    def recv(*names):
        for name in names:
            copies[name].wait_recv()

    al, ot = pl.ds(0, tokens), pl.ds(tokens, tokens)

    def place(c, par, q):
        if c in (0, 2):
            return pl.ds(par * tokens + q * quarter, quarter)
        return pl.ds((q % 2) * tokens + par * half + (q // 2) * quarter, quarter)

    for name, c_src, q, c_dst, device in (
            ('a1a', 0, 0, 1, right), ('a1b', 0, 1, 1, right), ('a2a', 0, 2, 1, left), ('a2b', 0, 3, 1, left),
            ('a3a', 0, 2, 2, right), ('a3b', 0, 3, 2, right), ('a4a', 0, 0, 2, left), ('a4b', 0, 1, 2, left),
            ('f1a', 1, 0, 3, right), ('f1b', 1, 1, 3, right), ('f2a', 1, 2, 3, left), ('f2b', 1, 3, 3, left)):
        remote(name, x_buf.at[c_src, place(c_src, 0, q)], x_buf.at[c_dst, place(c_dst, 0, q)], device)
    p_cols = [pl.ds(n * model // N_P, model // N_P) for n in range(N_P)]
    for c in (0, 2):
        remote(f'd{c}', x_buf.at[c, al], x_buf.at[c, ot], partner)
        for n, cols in enumerate(p_cols):
            remote(f'p{c}_{n}', p_buf.at[c, ot, cols], pr_buf.at[c, :, cols], partner)
    for c in (1, 3):
        for n, part in enumerate('ab'):
            remote(f'd{c}{part}', x_buf.at[c, pl.ds(n * tokens, half)], x_buf.at[c, pl.ds(n * tokens + half, half)], partner)
            remote(f'p{c}{part}', p_buf.at[c, pl.ds(n * tokens + half, half)], pr_buf.at[c, pl.ds(n * half, half)], partner)
    remote('g1', g_buf.at[0, 0], g_buf.at[1, 0], right)
    remote('g2', g_buf.at[0, 0], g_buf.at[2, 0], left)
    remote('g3', g_buf.at[1, 0], g_buf.at[3, 0], right)
    for c in range(4):
        remote(f'gd{c}', g_buf.at[c, 0], g_buf.at[c, 1], partner)
    for n, part in enumerate('ab'):
        for k, q, device in ((1, n, right), (2, n + 2, left)):
            rows = pl.ds(q * quarter, quarter)
            back = (q + 2) % 4
            remote(f'i{k}{part}', p_buf.at[1, place(1, 0, back)], near.at[pl.ds(back * quarter, quarter)], device)
            remote(f'o{k}{part}', p_buf.at[3, place(3, 0, q)], tb.at[rows], device)
            remote(f'w{k}{part}', p_buf.at[2, rows], far.at[rows], device)

    load('hid', hidden, v_hid)
    load('mn', moe_norm, v_mn)
    load('wr', w_router, v_wr)
    load('ids', ids, v_ids)
    load('an', attn_norm, v_an)
    load('wq', w_query, v_wq)
    load('wk', w_key, v_wk)
    load('wv', w_value, v_wv)
    load('fn', ffn_norm, v_fn)
    load('cos', cos_t, v_cos)
    load('sin', sin_t, v_sin)

    barrier = pltpu.get_barrier_semaphore()
    for peer in (partner, left, right):
        pl.semaphore_signal(barrier, inc=1, device_id={'ep': peer}, device_id_type=MESH)

    load('wo', w_out, v_wo)
    for e in range(n_local):
        load(f'eg{e}', exp_gate.at[e], v_eg.at[e])
        load(f'eu{e}', exp_up.at[e], v_eu.at[e])
    for e in range(n_local):
        load(f'ed{e}', exp_down.at[e], v_ed.at[e])

    def norm_row(ref):
        scale = ref[...].astype(F32)
        return jnp.concatenate([scale[r:r + 1] for r in range(scale.shape[0])], axis=1)

    ready('hid', 'mn')
    x_buf[0, :tokens] = rms_rows(v_hid[...], norm_row(v_mn))
    pl.semaphore_wait(barrier, 3)
    send('a1a', 'a2a', 'd0')

    ready('wr', 'ids')
    logits = lax.dot_general(v_wr[...], x_buf[0, :tokens], (((1,), (1,)), ((), ())), preferred_element_type=F32)
    expert_row = lax.broadcasted_iota(jnp.int32, logits.shape, 0)
    id_vals = v_ids[...]
    mask = expert_row == id_vals[0:1]
    for j in range(1, id_vals.shape[0]):
        mask = jnp.logical_or(mask, expert_row == id_vals[j:j + 1])
    top = jnp.max(jnp.where(mask, logits, -jnp.inf), axis=0, keepdims=True)
    powers = jnp.where(mask, jnp.exp(logits - top), 0.0)
    g_buf[0, 0] = powers / jnp.sum(powers, axis=0, keepdims=True)
    send('g1', 'g2', 'gd0', 'a1b', 'a2b', 'a3a', 'a4a')

    ready('an', 'wq', 'wk', 'wv', 'cos', 'sin')
    normed = rms_rows(v_hid[...], norm_row(v_an))
    qf[...] = dot(normed, v_wq[...])
    kf[...] = dot(normed, v_wk[...])
    vf[...] = dot(normed, v_wv[...])

    lane = lax.broadcasted_iota(jnp.int32, (tokens, LANES), 1)
    low_half = lax.rem(lane, 64) < 32
    head0 = lane < 64
    row = lax.rem(lax.broadcasted_iota(jnp.int32, (2 * tokens, tokens), 0), tokens)
    causal = row >= lax.broadcasted_iota(jnp.int32, (2 * tokens, tokens), 1)

    def rope(x):
        swapped = jnp.where(low_half, pltpu.roll(x, LANES - 32, 1), pltpu.roll(x, 32, 1))
        return x * v_cos[...] + swapped * v_sin[...]

    def attend(t):
        kt = rope(kf[:, t * LANES:(t + 1) * LANES])
        vt = vf[:, t * LANES:(t + 1) * LANES]
        kt_r, vt_r = pltpu.roll(kt, 64, 1), pltpu.roll(vt, 64, 1)
        for s in range(2):
            g = 2 * t + s
            k2 = (jnp.where(head0, kt, kt_r) if s == 0 else jnp.where(head0, kt_r, kt)).astype(BF16)
            v2 = (jnp.where(head0, vt, vt_r) if s == 0 else jnp.where(head0, vt_r, vt)).astype(BF16)
            q = rope(qf[:, g * LANES:(g + 1) * LANES])
            q2 = jnp.concatenate([jnp.where(head0, q, 0.0), jnp.where(head0, 0.0, q)], axis=0).astype(BF16)
            scores = lax.dot_general(q2, k2, (((1,), (1,)), ((), ())), preferred_element_type=F32) * 64 ** -0.5
            scores = jnp.where(causal, scores, -jnp.inf)
            prob = jnp.exp(scores - jnp.max(scores, axis=-1, keepdims=True))
            prob = (prob / jnp.sum(prob, axis=-1, keepdims=True)).astype(BF16)
            both = dot(prob, v2)
            ctx[:, g * LANES:(g + 1) * LANES] = jnp.where(head0, both[:tokens], both[tokens:]).astype(BF16)

    e_lane = lax.broadcasted_iota(jnp.int32, (tokens, n_experts), 1) - me * n_local
    t_lane = lax.broadcasted_iota(jnp.int32, (n_experts, tokens), 1) < half

    def set_gates(c, par):
        if c == 0:
            gt = g_buf[0, par]
        elif c == 3:
            gt = g_buf[3, par]
        elif c == 1:
            gt = jnp.where(t_lane, g_buf[1, par], g_buf[2, par])
        else:
            gt = jnp.where(t_lane, g_buf[2, par], g_buf[1, par])
        gates_c = gt.T
        for e in range(n_local):
            gate = jnp.sum(jnp.where(e_lane == e, gates_c, 0.0), axis=-1, keepdims=True)
            gate = jnp.broadcast_to(gate, (tokens, LANES))
            for q in range(4):
                gate_b[e, place(c, par, q)] = gate[q * quarter:(q + 1) * quarter]

    def act(c, rows, e):
        x = x_buf[c, rows]
        used = jnp.concatenate([gate_b[e, rows]] * (COL // LANES), axis=1) > 0.0
        for n in range(exp_ff // COL):
            cols = slice(n * COL, (n + 1) * COL)
            z = silu(dot(x, v_eg[e, :, cols])) * dot(x, v_eu[e, :, cols])
            hb[rows, e * exp_ff + n * COL:e * exp_ff + (n + 1) * COL] = jnp.where(used, z, 0.0).astype(BF16)

    def down(c, rows, col_lo, col_hi):
        for n in range(col_lo // COL, col_hi // COL):
            cols = slice(n * COL, (n + 1) * COL)
            for e in range(n_local):
                y = dot(hb[rows, e * exp_ff:(e + 1) * exp_ff], v_ed[e, :, cols]).astype(BF16).astype(F32)
                y = y * jnp.concatenate([gate_b[e, rows]] * (COL // LANES), axis=1)
                p_buf[c, rows, cols] = y if e == 0 else p_buf[c, rows, cols] + y

    def down_cols(c):
        for n in range(N_P):
            down(c, both, n * model // N_P, (n + 1) * model // N_P)
            send(f'p{c}_{n}')

    def down_rows(c, n):
        down(c, slice(n * tokens, (n + 1) * tokens), 0, model)
        send(f'p{c}' + 'ab'[n])

    def add_cols(c):
        for n in range(N_P):
            recv(f'p{c}_{n}')
        p_buf[c, :tokens] = p_buf[c, :tokens] + pr_buf[c]

    def add_rows(c, n):
        recv(f'p{c}' + 'ab'[n])
        rows = slice(n * tokens, n * tokens + half)
        p_buf[c, rows] = p_buf[c, rows] + pr_buf[c, n * half:(n + 1) * half]

    def send_near(n):
        add_rows(1, n)
        send('i1' + 'ab'[n], 'i2' + 'ab'[n])

    def send_far(n):
        add_rows(3, n)
        send('o1' + 'ab'[n], 'o2' + 'ab'[n])

    def pass_on(n):
        recv('o1' + 'ab'[n], 'o2' + 'ab'[n])
        for q in (n, n + 2):
            rows = slice(q * quarter, (q + 1) * quarter)
            p_buf[2, rows] = p_buf[2, rows] + tb[rows]
        send('w1' + 'ab'[n], 'w2' + 'ab'[n])

    def ffn_block(b, x):
        act_cols = slice(b * FF_BLOCK, (b + 1) * FF_BLOCK)
        for n in range(FF_BLOCK // COL):
            cols = slice(b * FF_BLOCK + n * COL, b * FF_BLOCK + (n + 1) * COL)
            z = silu(dot(x, v_fg[:, cols])) * dot(x, v_fu[:, cols])
            hb[:tokens, n * COL:(n + 1) * COL] = z.astype(BF16)
        h = hb[:tokens, :FF_BLOCK]
        for n in range(model // COL):
            cols = slice(n * COL, (n + 1) * COL)
            y = dot(h, v_fd[act_cols, cols])
            ffn_acc[:, cols] = y + (att[:, cols].astype(F32) if b == 0 else ffn_acc[:, cols])

    first, second, both = slice(0, tokens), slice(tokens, 2 * tokens), slice(0, 2 * tokens)
    attend(0)
    attend(1)
    attend(2)
    recv('a1a', 'a2a')
    send('f1a', 'f2a', 'd1a')
    recv('g1', 'g2')
    send('g3', 'gd1', 'gd2')
    attend(3)
    ready('wo', 'fn')
    att[...] = (v_hid[...].astype(F32) + dot(ctx[...], v_wo[...])).astype(BF16)

    n_blk = ff_dim // 1024
    for b in range(n_blk):
        cols = pl.ds(b * 1024, 1024)
        load(f'fg{b}', ffn_gate.at[:, cols], v_fg.at[:, cols])
        load(f'fu{b}', ffn_up.at[:, cols], v_fu.at[:, cols])
        load(f'fd{b}', ffn_down.at[cols], v_fd.at[cols])

    for e in range(n_local):
        ready(f'eg{e}', f'eu{e}', f'ed{e}')
    recv('gd1', 'gd2', 'd1a')
    set_gates(1, 0)
    set_gates(1, 1)
    act(1, first, 0)
    recv('a1b', 'a2b')
    send('f1b', 'f2b', 'd1b', 'a3b', 'a4b')
    for e in range(1, n_local):
        act(1, first, e)
    down_rows(1, 0)
    recv('d1b')
    for e in range(n_local - 1):
        act(1, second, e)
    recv('f1a', 'f2a', 'g3')
    send('d3a', 'gd3')
    act(1, second, n_local - 1)
    send_near(0)
    down_rows(1, 1)
    recv('gd3', 'd3a')
    set_gates(3, 0)
    set_gates(3, 1)
    act(3, first, 0)
    act(3, first, 1)
    recv('f1b', 'f2b')
    send('d3b')
    act(3, first, 2)
    act(3, first, 3)
    send_near(1)
    down_rows(3, 0)
    recv('d3b', 'a3a', 'a3b', 'a4a', 'a4b')
    send('d2')
    for e in range(n_local):
        act(3, second, e)
    send_far(0)
    down_rows(3, 1)
    recv('d2')
    set_gates(2, 0)
    set_gates(2, 1)
    act(2, both, 0)
    act(2, both, 1)
    send_far(1)
    act(2, both, 2)
    act(2, both, 3)
    down_cols(2)
    recv('d0', 'gd0')
    set_gates(0, 0)
    set_gates(0, 1)
    act(0, both, 0)
    act(0, both, 1)
    add_cols(2)
    pass_on(0)
    act(0, both, 2)
    act(0, both, 3)
    down_cols(0)
    for b in range(n_blk):
        ready(f'fg{b}', f'fu{b}', f'fd{b}')
    pass_on(1)
    normed_ffn = rms_rows(att[...], norm_row(v_fn))
    for b in range(ff_dim // FF_BLOCK):
        ffn_block(b, normed_ffn)
    add_cols(0)
    recv('i1a', 'i2a', 'i1b', 'i2b')
    late = ('w1a', 'w2a', 'w1b', 'w2b')
    for name, copy in copies.items():
        if name not in late:
            copy.wait_send()
    total[...] = ffn_acc[...] + p_buf[0, :tokens] + near[...]
    for name in late:
        copies[name].wait_recv()
        copies[name].wait_send()


def solution(mesh):
    group = mesh.shape['ep']
    row_spec = P(('dp', 'ep'), None, None)
    vec_spec = P(None)
    mat_spec = P(None, None)
    cube_spec = P(None, None, None)
    expert_spec = P('ep', None, None)

    def per_device(hidden, expert_ids, slot_ids, attn_norm, w_query, w_key, w_value, w_out, ffn_norm, ffn_gate, ffn_up, ffn_down, moe_norm, w_router, exp_gate, exp_up, exp_down):
        n_seqs, seq_len, model = hidden.shape
        tokens = n_seqs * seq_len
        n_heads, head_dim = w_out.shape[0], w_out.shape[1]
        top_k = expert_ids.shape[-1]
        n_local, _, exp_ff = exp_gate.shape
        n_experts = w_router.shape[1]
        kv_dim = w_key.shape[1]
        assert n_seqs == 1 and group == 8 and head_dim == 64
        cos_t, sin_t = rope_tables(seq_len, head_dim)
        args = (hidden.reshape(tokens, model), expert_ids.reshape(tokens, top_k).T, attn_norm.reshape(-1, LANES),
                w_query, w_key, w_value, w_out.reshape(n_heads * head_dim, model), ffn_norm.reshape(-1, LANES),
                ffn_gate, ffn_up, ffn_down, moe_norm.reshape(-1, LANES), w_router.T, exp_gate, exp_up, exp_down,
                jnp.asarray(cos_t), jnp.asarray(sin_t))
        vmem = [pltpu.VMEM(a.shape, a.dtype) for a in args]
        scratch = vmem + [
            pltpu.VMEM((4, 2 * tokens, model), BF16),
            pltpu.VMEM((4, 2, n_experts, tokens), F32),
            pltpu.VMEM((4, 2 * tokens, model), F32),
            pltpu.VMEM((4, tokens, model), F32),
            pltpu.VMEM((tokens, model), F32),
            pltpu.VMEM((tokens, model), F32),
            pltpu.VMEM((tokens, n_heads * head_dim), F32),
            pltpu.VMEM((tokens, kv_dim), F32),
            pltpu.VMEM((tokens, kv_dim), F32),
            pltpu.VMEM((tokens, n_heads * head_dim), BF16),
            pltpu.VMEM((2 * tokens, n_local * exp_ff), BF16),
            pltpu.VMEM((n_local, 2 * tokens, LANES), F32),
            pltpu.VMEM((tokens, model), BF16),
            pltpu.VMEM((tokens, model), F32),
            pltpu.SemaphoreType.DMA((48,)),
            pltpu.SemaphoreType.DMA((64,)),
            pltpu.SemaphoreType.DMA((64,)),
        ]
        total, far = pl.pallas_call(
            functools.partial(kernel, group),
            out_shape=(pltpu.VMEM((tokens, model), F32), pltpu.VMEM((tokens, model), F32)),
            in_specs=[pl.BlockSpec(memory_space=pl.ANY)] * len(args),
            out_specs=(pl.BlockSpec(memory_space=pltpu.VMEM),) * 2,
            scratch_shapes=scratch,
            compiler_params=pltpu.CompilerParams(collective_id=0, has_side_effects=True, vmem_limit_bytes=VMEM_BYTES),
        )(*args)
        return (total + far).astype(BF16).reshape(n_seqs, seq_len, model)

    return jax.shard_map(per_device, mesh=mesh, in_specs=(row_spec, row_spec, row_spec, vec_spec, mat_spec, mat_spec, mat_spec, cube_spec, vec_spec, mat_spec, mat_spec, mat_spec, vec_spec, mat_spec, expert_spec, expert_spec, expert_spec), out_specs=row_spec, check_vma=False)
```

```python
import functools

import jax
import jax.numpy as jnp
import numpy as np
from jax import lax
from jax.experimental import pallas as pl
from jax.experimental.pallas import tpu as pltpu
from jax.sharding import PartitionSpec as P

RMS_EPS = 1e-6
ROPE_BASE = 10000.0
MESH = pl.DeviceIdType.MESH
F32, BF16 = jnp.float32, jnp.bfloat16
LANES = 128
FF_BLOCK = 512
COL = 256
N_P = 2
VMEM_BYTES = 60 * 1024 * 1024


def rms_rows(row_vals, norm_scale):
    as_float = row_vals.astype(F32)
    inv_rms = lax.rsqrt(jnp.mean(as_float * as_float, axis=-1, keepdims=True) + RMS_EPS)
    return (as_float * inv_rms * norm_scale).astype(BF16)


def silu(z):
    half = 0.5 * z
    return half + half * jnp.tanh(half)


def dot(a, b):
    return jnp.dot(a, b, preferred_element_type=F32)


def rope_tables(seq_len, head_dim):
    half = head_dim // 2
    lane = np.arange(LANES)
    freq = ROPE_BASE ** (-2.0 * (lane % half) / head_dim)
    angle = np.arange(seq_len)[:, None] * freq[None, :]
    sign = np.where(lane % head_dim < half, -1.0, 1.0)
    return np.cos(angle).astype(np.float32), (np.sin(angle) * sign[None, :]).astype(np.float32)


def kernel(group, hidden, ids, attn_norm, w_query, w_key, w_value, w_out, ffn_norm, ffn_gate, ffn_up, ffn_down,
           moe_norm, w_router, exp_gate, exp_up, exp_down, cos_t, sin_t, total, far,
           v_hid, v_ids, v_an, v_wq, v_wk, v_wv, v_wo, v_fn, v_fg, v_fu, v_fd, v_mn, v_wr, v_eg, v_eu, v_ed, v_cos, v_sin,
           x_buf, g_buf, p_buf, pr_buf, tb, near, qf, kf, vf, ctx, hb, gate_b, att, ffn_acc,
           w_sem, s_sem, r_sem):
    tokens, model = v_hid.shape
    half, quarter = tokens // 2, tokens // 4
    n_local = v_eg.shape[0]
    exp_ff = v_eg.shape[2]
    ff_dim = v_fg.shape[1]
    n_experts = v_wr.shape[0]
    me = lax.axis_index('ep')
    partner = me + 1 - 2 * lax.rem(me, 2)
    right = lax.rem(me + 2, group)
    left = lax.rem(me + group - 2, group)

    loads = {}

    def load(name, src, dst):
        loads[name] = pltpu.make_async_copy(src, dst, w_sem.at[len(loads)])
        loads[name].start()

    def ready(*names):
        for name in names:
            loads[name].wait()

    copies = {}

    def remote(name, src, dst, device):
        k = len(copies)
        copies[name] = pltpu.make_async_remote_copy(
            src_ref=src, dst_ref=dst, send_sem=s_sem.at[k], recv_sem=r_sem.at[k],
            device_id={'ep': device}, device_id_type=MESH)

    def send(*names):
        for name in names:
            copies[name].start()

    def recv(*names):
        for name in names:
            copies[name].wait_recv()

    al, ot = pl.ds(0, tokens), pl.ds(tokens, tokens)

    def place(c, par, q):
        if c in (0, 2):
            return pl.ds(par * tokens + q * quarter, quarter)
        return pl.ds((q % 2) * tokens + par * half + (q // 2) * quarter, quarter)

    for name, c_src, q, c_dst, device in (
            ('a1a', 0, 0, 1, right), ('a1b', 0, 1, 1, right), ('a2a', 0, 2, 1, left), ('a2b', 0, 3, 1, left),
            ('a3a', 0, 2, 2, right), ('a3b', 0, 3, 2, right), ('a4a', 0, 0, 2, left), ('a4b', 0, 1, 2, left),
            ('f1a', 1, 0, 3, right), ('f1b', 1, 1, 3, right), ('f2a', 1, 2, 3, left), ('f2b', 1, 3, 3, left)):
        remote(name, x_buf.at[c_src, place(c_src, 0, q)], x_buf.at[c_dst, place(c_dst, 0, q)], device)
    p_cols = [pl.ds(n * model // N_P, model // N_P) for n in range(N_P)]
    for c in (0, 2):
        remote(f'd{c}', x_buf.at[c, al], x_buf.at[c, ot], partner)
        for n, cols in enumerate(p_cols):
            remote(f'p{c}_{n}', p_buf.at[c, ot, cols], pr_buf.at[c, :, cols], partner)
    for c in (1, 3):
        for n, part in enumerate('ab'):
            remote(f'd{c}{part}', x_buf.at[c, pl.ds(n * tokens, half)], x_buf.at[c, pl.ds(n * tokens + half, half)], partner)
            remote(f'p{c}{part}', p_buf.at[c, pl.ds(n * tokens + half, half)], pr_buf.at[c, pl.ds(n * half, half)], partner)
    remote('g1', g_buf.at[0, 0], g_buf.at[1, 0], right)
    remote('g2', g_buf.at[0, 0], g_buf.at[2, 0], left)
    remote('g3', g_buf.at[1, 0], g_buf.at[3, 0], right)
    for c in range(4):
        remote(f'gd{c}', g_buf.at[c, 0], g_buf.at[c, 1], partner)
    for n, part in enumerate('ab'):
        for k, q, device in ((1, n, right), (2, n + 2, left)):
            rows = pl.ds(q * quarter, quarter)
            back = (q + 2) % 4
            remote(f'i{k}{part}', p_buf.at[1, place(1, 0, back)], near.at[pl.ds(back * quarter, quarter)], device)
            remote(f'o{k}{part}', p_buf.at[3, place(3, 0, q)], tb.at[rows], device)
            remote(f'w{k}{part}', p_buf.at[2, rows], far.at[rows], device)

    load('hid', hidden, v_hid)
    load('mn', moe_norm, v_mn)
    load('wr', w_router, v_wr)
    load('ids', ids, v_ids)
    load('an', attn_norm, v_an)
    load('wq', w_query, v_wq)
    load('wk', w_key, v_wk)
    load('wv', w_value, v_wv)
    load('fn', ffn_norm, v_fn)
    load('cos', cos_t, v_cos)
    load('sin', sin_t, v_sin)

    barrier = pltpu.get_barrier_semaphore()
    for peer in (partner, left, right):
        pl.semaphore_signal(barrier, inc=1, device_id={'ep': peer}, device_id_type=MESH)

    load('wo', w_out, v_wo)
    for e in range(n_local):
        load(f'eg{e}', exp_gate.at[e], v_eg.at[e])
        load(f'eu{e}', exp_up.at[e], v_eu.at[e])
    for e in range(n_local):
        load(f'ed{e}', exp_down.at[e], v_ed.at[e])

    def norm_row(ref):
        scale = ref[...].astype(F32)
        return jnp.concatenate([scale[r:r + 1] for r in range(scale.shape[0])], axis=1)

    ready('hid', 'mn')
    x_buf[0, :tokens] = rms_rows(v_hid[...], norm_row(v_mn))
    pl.semaphore_wait(barrier, 3)
    send('a1a', 'a2a', 'd0')

    ready('wr', 'ids')
    logits = lax.dot_general(v_wr[...], x_buf[0, :tokens], (((1,), (1,)), ((), ())), preferred_element_type=F32)
    expert_row = lax.broadcasted_iota(jnp.int32, logits.shape, 0)
    id_vals = v_ids[...]
    mask = expert_row == id_vals[0:1]
    for j in range(1, id_vals.shape[0]):
        mask = jnp.logical_or(mask, expert_row == id_vals[j:j + 1])
    top = jnp.max(jnp.where(mask, logits, -jnp.inf), axis=0, keepdims=True)
    powers = jnp.where(mask, jnp.exp(logits - top), 0.0)
    g_buf[0, 0] = powers / jnp.sum(powers, axis=0, keepdims=True)
    send('g1', 'g2', 'gd0', 'a1b', 'a2b', 'a3a', 'a4a')

    ready('an', 'wq', 'wk', 'wv', 'cos', 'sin')
    normed = rms_rows(v_hid[...], norm_row(v_an))
    qf[...] = dot(normed, v_wq[...])
    kf[...] = dot(normed, v_wk[...])
    vf[...] = dot(normed, v_wv[...])

    lane = lax.broadcasted_iota(jnp.int32, (tokens, LANES), 1)
    low_half = lax.rem(lane, 64) < 32
    head0 = lane < 64
    row = lax.rem(lax.broadcasted_iota(jnp.int32, (2 * tokens, tokens), 0), tokens)
    causal = row >= lax.broadcasted_iota(jnp.int32, (2 * tokens, tokens), 1)

    def rope(x):
        swapped = jnp.where(low_half, pltpu.roll(x, LANES - 32, 1), pltpu.roll(x, 32, 1))
        return x * v_cos[...] + swapped * v_sin[...]

    def attend(t):
        kt = rope(kf[:, t * LANES:(t + 1) * LANES])
        vt = vf[:, t * LANES:(t + 1) * LANES]
        kt_r, vt_r = pltpu.roll(kt, 64, 1), pltpu.roll(vt, 64, 1)
        for s in range(2):
            g = 2 * t + s
            k2 = (jnp.where(head0, kt, kt_r) if s == 0 else jnp.where(head0, kt_r, kt)).astype(BF16)
            v2 = (jnp.where(head0, vt, vt_r) if s == 0 else jnp.where(head0, vt_r, vt)).astype(BF16)
            q = rope(qf[:, g * LANES:(g + 1) * LANES])
            q2 = jnp.concatenate([jnp.where(head0, q, 0.0), jnp.where(head0, 0.0, q)], axis=0).astype(BF16)
            scores = lax.dot_general(q2, k2, (((1,), (1,)), ((), ())), preferred_element_type=F32) * 64 ** -0.5
            scores = jnp.where(causal, scores, -jnp.inf)
            prob = jnp.exp(scores - jnp.max(scores, axis=-1, keepdims=True))
            prob = (prob / jnp.sum(prob, axis=-1, keepdims=True)).astype(BF16)
            both = dot(prob, v2)
            ctx[:, g * LANES:(g + 1) * LANES] = jnp.where(head0, both[:tokens], both[tokens:]).astype(BF16)

    e_lane = lax.broadcasted_iota(jnp.int32, (tokens, n_experts), 1) - me * n_local
    t_lane = lax.broadcasted_iota(jnp.int32, (n_experts, tokens), 1) < half

    def set_gates(c, par):
        if c == 0:
            gt = g_buf[0, par]
        elif c == 3:
            gt = g_buf[3, par]
        elif c == 1:
            gt = jnp.where(t_lane, g_buf[1, par], g_buf[2, par])
        else:
            gt = jnp.where(t_lane, g_buf[2, par], g_buf[1, par])
        gates_c = gt.T
        for e in range(n_local):
            gate = jnp.sum(jnp.where(e_lane == e, gates_c, 0.0), axis=-1, keepdims=True)
            gate = jnp.broadcast_to(gate, (tokens, LANES))
            for q in range(4):
                gate_b[int(c == 0), e, place(c, par, q)] = gate[q * quarter:(q + 1) * quarter]

    def act(c, rows, e):
        x = x_buf[c, rows]
        used = jnp.concatenate([gate_b[int(c == 0), e, rows]] * (COL // LANES), axis=1) > 0.0
        for n in range(exp_ff // COL):
            cols = slice(n * COL, (n + 1) * COL)
            z = silu(dot(x, v_eg[e, :, cols])) * dot(x, v_eu[e, :, cols])
            hb[int(c == 0), rows, e * exp_ff + n * COL:e * exp_ff + (n + 1) * COL] = jnp.where(used, z, 0.0).astype(BF16)

    def down(c, rows, col_lo, col_hi):
        for n in range(col_lo // COL, col_hi // COL):
            cols = slice(n * COL, (n + 1) * COL)
            for e in range(n_local):
                y = dot(hb[int(c == 0), rows, e * exp_ff:(e + 1) * exp_ff], v_ed[e, :, cols]).astype(BF16).astype(F32)
                y = y * jnp.concatenate([gate_b[int(c == 0), e, rows]] * (COL // LANES), axis=1)
                p_buf[c, rows, cols] = y if e == 0 else p_buf[c, rows, cols] + y

    def down_cols(c):
        for n in range(N_P):
            down(c, both, n * model // N_P, (n + 1) * model // N_P)
            send(f'p{c}_{n}')

    def down_rows(c, n):
        down(c, slice(n * tokens, (n + 1) * tokens), 0, model)
        send(f'p{c}' + 'ab'[n])

    def add_cols(c):
        for n in range(N_P):
            recv(f'p{c}_{n}')
        p_buf[c, :tokens] = p_buf[c, :tokens] + pr_buf[c]

    def add_rows(c, n):
        recv(f'p{c}' + 'ab'[n])
        rows = slice(n * tokens, n * tokens + half)
        p_buf[c, rows] = p_buf[c, rows] + pr_buf[c, n * half:(n + 1) * half]

    def send_near(n):
        add_rows(1, n)
        send('i1' + 'ab'[n], 'i2' + 'ab'[n])

    def send_far(n):
        add_rows(3, n)
        send('o1' + 'ab'[n], 'o2' + 'ab'[n])

    def pass_on(n):
        recv('o1' + 'ab'[n], 'o2' + 'ab'[n])
        for q in (n, n + 2):
            rows = slice(q * quarter, (q + 1) * quarter)
            p_buf[2, rows] = p_buf[2, rows] + tb[rows]
        send('w1' + 'ab'[n], 'w2' + 'ab'[n])

    def ffn_block(b, x):
        act_cols = slice(b * FF_BLOCK, (b + 1) * FF_BLOCK)
        for n in range(FF_BLOCK // COL):
            cols = slice(b * FF_BLOCK + n * COL, b * FF_BLOCK + (n + 1) * COL)
            z = silu(dot(x, v_fg[:, cols])) * dot(x, v_fu[:, cols])
            hb[0, :tokens, n * COL:(n + 1) * COL] = z.astype(BF16)
        h = hb[0, :tokens, :FF_BLOCK]
        for n in range(model // COL):
            cols = slice(n * COL, (n + 1) * COL)
            y = dot(h, v_fd[act_cols, cols])
            ffn_acc[:, cols] = y + (att[:, cols].astype(F32) if b == 0 else ffn_acc[:, cols])

    first, second, both = slice(0, tokens), slice(tokens, 2 * tokens), slice(0, 2 * tokens)
    attend(0)
    attend(1)
    attend(2)
    recv('a1a', 'a2a')
    send('f1a', 'f2a', 'd1a')
    attend(3)
    recv('g1', 'g2')
    send('g3', 'gd1', 'gd2')
    ready('wo', 'fn')
    att[...] = (v_hid[...].astype(F32) + dot(ctx[...], v_wo[...])).astype(BF16)

    n_blk = ff_dim // 1024
    for b in range(n_blk):
        cols = pl.ds(b * 1024, 1024)
        load(f'fg{b}', ffn_gate.at[:, cols], v_fg.at[:, cols])
        load(f'fu{b}', ffn_up.at[:, cols], v_fu.at[:, cols])
        load(f'fd{b}', ffn_down.at[cols], v_fd.at[cols])

    ready('eg0', 'eu0')
    recv('d0', 'gd0')
    set_gates(0, 0)
    set_gates(0, 1)
    act(0, both, 0)
    for e in range(1, n_local):
        ready(f'eg{e}', f'eu{e}')
    recv('gd1', 'gd2', 'd1a')
    set_gates(1, 0)
    set_gates(1, 1)
    act(1, first, 0)
    recv('a1b', 'a2b')
    send('f1b', 'f2b', 'd1b', 'a3b', 'a4b')
    for e in range(1, n_local):
        act(1, first, e)
    for e in range(n_local):
        ready(f'ed{e}')
    down_rows(1, 0)
    recv('d1b')
    for e in range(n_local - 1):
        act(1, second, e)
    recv('f1a', 'f2a', 'g3')
    send('d3a', 'gd3')
    act(1, second, n_local - 1)
    send_near(0)
    down_rows(1, 1)
    recv('gd3', 'd3a')
    set_gates(3, 0)
    set_gates(3, 1)
    act(3, first, 0)
    act(3, first, 1)
    recv('f1b', 'f2b')
    send('d3b')
    act(3, first, 2)
    act(3, first, 3)
    send_near(1)
    down_rows(3, 0)
    recv('d3b', 'a3a', 'a3b', 'a4a', 'a4b')
    send('d2')
    for e in range(n_local):
        act(3, second, e)
    send_far(0)
    down_rows(3, 1)
    recv('d2')
    set_gates(2, 0)
    set_gates(2, 1)
    act(2, both, 0)
    act(2, both, 1)
    send_far(1)
    act(2, both, 2)
    act(2, both, 3)
    down_cols(2)
    act(0, both, 1)
    act(0, both, 2)
    add_cols(2)
    pass_on(0)
    act(0, both, 3)
    down_cols(0)
    for b in range(n_blk):
        ready(f'fg{b}', f'fu{b}', f'fd{b}')
    pass_on(1)
    normed_ffn = rms_rows(att[...], norm_row(v_fn))
    for b in range(ff_dim // FF_BLOCK):
        ffn_block(b, normed_ffn)
    add_cols(0)
    recv('i1a', 'i2a', 'i1b', 'i2b')
    late = ('w1a', 'w2a', 'w1b', 'w2b')
    for name, copy in copies.items():
        if name not in late:
            copy.wait_send()
    total[...] = ffn_acc[...] + p_buf[0, :tokens] + near[...]
    for name in late:
        copies[name].wait_recv()
        copies[name].wait_send()


def solution(mesh):
    group = mesh.shape['ep']
    row_spec = P(('dp', 'ep'), None, None)
    vec_spec = P(None)
    mat_spec = P(None, None)
    cube_spec = P(None, None, None)
    expert_spec = P('ep', None, None)

    def per_device(hidden, expert_ids, slot_ids, attn_norm, w_query, w_key, w_value, w_out, ffn_norm, ffn_gate, ffn_up, ffn_down, moe_norm, w_router, exp_gate, exp_up, exp_down):
        n_seqs, seq_len, model = hidden.shape
        tokens = n_seqs * seq_len
        n_heads, head_dim = w_out.shape[0], w_out.shape[1]
        top_k = expert_ids.shape[-1]
        n_local, _, exp_ff = exp_gate.shape
        n_experts = w_router.shape[1]
        kv_dim = w_key.shape[1]
        assert n_seqs == 1 and group == 8 and head_dim == 64
        cos_t, sin_t = rope_tables(seq_len, head_dim)
        args = (hidden.reshape(tokens, model), expert_ids.reshape(tokens, top_k).T, attn_norm.reshape(-1, LANES),
                w_query, w_key, w_value, w_out.reshape(n_heads * head_dim, model), ffn_norm.reshape(-1, LANES),
                ffn_gate, ffn_up, ffn_down, moe_norm.reshape(-1, LANES), w_router.T, exp_gate, exp_up, exp_down,
                jnp.asarray(cos_t), jnp.asarray(sin_t))
        vmem = [pltpu.VMEM(a.shape, a.dtype) for a in args]
        scratch = vmem + [
            pltpu.VMEM((4, 2 * tokens, model), BF16),
            pltpu.VMEM((4, 2, n_experts, tokens), F32),
            pltpu.VMEM((4, 2 * tokens, model), F32),
            pltpu.VMEM((4, tokens, model), F32),
            pltpu.VMEM((tokens, model), F32),
            pltpu.VMEM((tokens, model), F32),
            pltpu.VMEM((tokens, n_heads * head_dim), F32),
            pltpu.VMEM((tokens, kv_dim), F32),
            pltpu.VMEM((tokens, kv_dim), F32),
            pltpu.VMEM((tokens, n_heads * head_dim), BF16),
            pltpu.VMEM((2, 2 * tokens, n_local * exp_ff), BF16),
            pltpu.VMEM((2, n_local, 2 * tokens, LANES), F32),
            pltpu.VMEM((tokens, model), BF16),
            pltpu.VMEM((tokens, model), F32),
            pltpu.SemaphoreType.DMA((48,)),
            pltpu.SemaphoreType.DMA((64,)),
            pltpu.SemaphoreType.DMA((64,)),
        ]
        total, far = pl.pallas_call(
            functools.partial(kernel, group),
            out_shape=(pltpu.VMEM((tokens, model), F32), pltpu.VMEM((tokens, model), F32)),
            in_specs=[pl.BlockSpec(memory_space=pl.ANY)] * len(args),
            out_specs=(pl.BlockSpec(memory_space=pltpu.VMEM),) * 2,
            scratch_shapes=scratch,
            compiler_params=pltpu.CompilerParams(collective_id=0, has_side_effects=True, vmem_limit_bytes=VMEM_BYTES),
        )(*args)
        return (total + far).astype(BF16).reshape(n_seqs, seq_len, model)

    return jax.shard_map(per_device, mesh=mesh, in_specs=(row_spec, row_spec, row_spec, vec_spec, mat_spec, mat_spec, mat_spec, cube_spec, vec_spec, mat_spec, mat_spec, mat_spec, vec_spec, mat_spec, expert_spec, expert_spec, expert_spec), out_specs=row_spec, check_vma=False)
```

```python
import functools

import jax
import jax.numpy as jnp
import numpy as np
from jax import lax
from jax.experimental import pallas as pl
from jax.experimental.pallas import tpu as pltpu
from jax.sharding import PartitionSpec as P

RMS_EPS = 1e-6
ROPE_BASE = 10000.0
MESH = pl.DeviceIdType.MESH
F32, BF16 = jnp.float32, jnp.bfloat16
LANES = 128
FF_BLOCK = 512
COL = 256
N_P = 2
VMEM_BYTES = 60 * 1024 * 1024


def rms_rows(row_vals, norm_scale):
    as_float = row_vals.astype(F32)
    inv_rms = lax.rsqrt(jnp.mean(as_float * as_float, axis=-1, keepdims=True) + RMS_EPS)
    return (as_float * inv_rms * norm_scale).astype(BF16)


def silu(z):
    half = 0.5 * z
    return half + half * jnp.tanh(half)


def dot(a, b):
    return jnp.dot(a, b, preferred_element_type=F32)


def rope_tables(seq_len, head_dim):
    half = head_dim // 2
    lane = np.arange(LANES)
    freq = ROPE_BASE ** (-2.0 * (lane % half) / head_dim)
    angle = np.arange(seq_len)[:, None] * freq[None, :]
    sign = np.where(lane % head_dim < half, -1.0, 1.0)
    return np.cos(angle).astype(np.float32), (np.sin(angle) * sign[None, :]).astype(np.float32)


def kernel(group, hidden, ids, attn_norm, w_query, w_key, w_value, w_out, ffn_norm, ffn_gate, ffn_up, ffn_down,
           moe_norm, w_router, exp_gate, exp_up, exp_down, cos_t, sin_t, total, far,
           v_hid, v_ids, v_an, v_wq, v_wk, v_wv, v_wo, v_fn, v_fg, v_fu, v_fd, v_mn, v_wr, v_eg, v_eu, v_ed, v_cos, v_sin,
           x_buf, g_buf, p_buf, pr_buf, tb, near, qf, kf, vf, ctx, hb, gate_b, att, ffn_acc,
           w_sem, s_sem, r_sem):
    tokens, model = v_hid.shape
    half, quarter = tokens // 2, tokens // 4
    n_local = v_eg.shape[0]
    exp_ff = v_eg.shape[2]
    ff_dim = v_fg.shape[1]
    n_experts = v_wr.shape[0]
    me = lax.axis_index('ep')
    partner = me + 1 - 2 * lax.rem(me, 2)
    right = lax.rem(me + 2, group)
    left = lax.rem(me + group - 2, group)

    loads = {}

    def load(name, src, dst):
        loads[name] = pltpu.make_async_copy(src, dst, w_sem.at[len(loads)])
        loads[name].start()

    def ready(*names):
        for name in names:
            loads[name].wait()

    copies = {}

    def remote(name, src, dst, device):
        k = len(copies)
        copies[name] = pltpu.make_async_remote_copy(
            src_ref=src, dst_ref=dst, send_sem=s_sem.at[k], recv_sem=r_sem.at[k],
            device_id={'ep': device}, device_id_type=MESH)

    def send(*names):
        for name in names:
            copies[name].start()

    def recv(*names):
        for name in names:
            copies[name].wait_recv()

    al, ot = pl.ds(0, tokens), pl.ds(tokens, tokens)

    def place(c, par, q):
        if c == 0:
            return pl.ds(par * tokens + q * quarter, quarter)
        return pl.ds((q % 2) * tokens + par * half + (q // 2) * quarter, quarter)

    for name, c_src, q, c_dst, device in (
            ('a1a', 0, 0, 1, right), ('a1b', 0, 1, 1, right), ('a2a', 0, 2, 1, left), ('a2b', 0, 3, 1, left),
            ('a3a', 0, 2, 2, right), ('a3b', 0, 3, 2, right), ('a4a', 0, 0, 2, left), ('a4b', 0, 1, 2, left),
            ('f1a', 1, 0, 3, right), ('f1b', 1, 1, 3, right), ('f2a', 1, 2, 3, left), ('f2b', 1, 3, 3, left)):
        remote(name, x_buf.at[c_src, place(c_src, 0, q)], x_buf.at[c_dst, place(c_dst, 0, q)], device)
    p_cols = [pl.ds(n * model // N_P, model // N_P) for n in range(N_P)]
    remote('d0', x_buf.at[0, al], x_buf.at[0, ot], partner)
    for n, cols in enumerate(p_cols):
        remote(f'p0_{n}', p_buf.at[0, ot, cols], pr_buf.at[0, :, cols], partner)
    for c in (1, 2, 3):
        for n, part in enumerate('ab'):
            remote(f'd{c}{part}', x_buf.at[c, pl.ds(n * tokens, half)], x_buf.at[c, pl.ds(n * tokens + half, half)], partner)
            remote(f'p{c}{part}', p_buf.at[c, pl.ds(n * tokens + half, half)], pr_buf.at[c, pl.ds(n * half, half)], partner)
    remote('g1', g_buf.at[0, 0], g_buf.at[1, 0], right)
    remote('g2', g_buf.at[0, 0], g_buf.at[2, 0], left)
    remote('g3', g_buf.at[1, 0], g_buf.at[3, 0], right)
    for c in range(4):
        remote(f'gd{c}', g_buf.at[c, 0], g_buf.at[c, 1], partner)
    for n, part in enumerate('ab'):
        for k, q, device in ((1, n, right), (2, n + 2, left)):
            rows = pl.ds(q * quarter, quarter)
            back = (q + 2) % 4
            remote(f'i{k}{part}', p_buf.at[1, place(1, 0, back)], near.at[pl.ds(back * quarter, quarter)], device)
            remote(f'o{k}{part}', p_buf.at[3, place(3, 0, q)], tb.at[rows], device)
            remote(f'w{k}{part}', p_buf.at[2, place(2, 0, q)], far.at[rows], device)

    load('hid', hidden, v_hid)
    load('mn', moe_norm, v_mn)
    load('wr', w_router, v_wr)
    load('ids', ids, v_ids)
    load('an', attn_norm, v_an)
    load('wq', w_query, v_wq)
    load('wk', w_key, v_wk)
    load('wv', w_value, v_wv)
    load('fn', ffn_norm, v_fn)
    load('cos', cos_t, v_cos)
    load('sin', sin_t, v_sin)

    barrier = pltpu.get_barrier_semaphore()
    for peer in (partner, left, right):
        pl.semaphore_signal(barrier, inc=1, device_id={'ep': peer}, device_id_type=MESH)

    for e in range(n_local):
        load(f'eg{e}', exp_gate.at[e], v_eg.at[e])
        load(f'eu{e}', exp_up.at[e], v_eu.at[e])
    for e in range(n_local):
        load(f'ed{e}', exp_down.at[e], v_ed.at[e])
    load('wo', w_out, v_wo)

    def norm_row(ref):
        scale = ref[...].astype(F32)
        return jnp.concatenate([scale[r:r + 1] for r in range(scale.shape[0])], axis=1)

    ready('hid', 'mn')
    x_buf[0, :tokens] = rms_rows(v_hid[...], norm_row(v_mn))
    pl.semaphore_wait(barrier, 3)
    send('a1a', 'a2a', 'd0')

    ready('wr', 'ids')
    logits = lax.dot_general(v_wr[...], x_buf[0, :tokens], (((1,), (1,)), ((), ())), preferred_element_type=F32)
    expert_row = lax.broadcasted_iota(jnp.int32, logits.shape, 0)
    id_vals = v_ids[...]
    mask = expert_row == id_vals[0:1]
    for j in range(1, id_vals.shape[0]):
        mask = jnp.logical_or(mask, expert_row == id_vals[j:j + 1])
    top = jnp.max(jnp.where(mask, logits, -jnp.inf), axis=0, keepdims=True)
    powers = jnp.where(mask, jnp.exp(logits - top), 0.0)
    g_buf[0, 0] = powers / jnp.sum(powers, axis=0, keepdims=True)
    send('g1', 'g2', 'gd0', 'a1b', 'a2b', 'a3a', 'a4a')

    ready('an', 'wq', 'wk', 'wv', 'cos', 'sin')
    normed = rms_rows(v_hid[...], norm_row(v_an))
    qf[...] = dot(normed, v_wq[...])
    kf[...] = dot(normed, v_wk[...])
    vf[...] = dot(normed, v_wv[...])

    lane = lax.broadcasted_iota(jnp.int32, (tokens, LANES), 1)
    low_half = lax.rem(lane, 64) < 32
    head0 = lane < 64
    row = lax.rem(lax.broadcasted_iota(jnp.int32, (2 * tokens, tokens), 0), tokens)
    causal = row >= lax.broadcasted_iota(jnp.int32, (2 * tokens, tokens), 1)

    def rope(x):
        swapped = jnp.where(low_half, pltpu.roll(x, LANES - 32, 1), pltpu.roll(x, 32, 1))
        return x * v_cos[...] + swapped * v_sin[...]

    def attend(t):
        kt = rope(kf[:, t * LANES:(t + 1) * LANES])
        vt = vf[:, t * LANES:(t + 1) * LANES]
        kt_r, vt_r = pltpu.roll(kt, 64, 1), pltpu.roll(vt, 64, 1)
        for s in range(2):
            g = 2 * t + s
            k2 = (jnp.where(head0, kt, kt_r) if s == 0 else jnp.where(head0, kt_r, kt)).astype(BF16)
            v2 = (jnp.where(head0, vt, vt_r) if s == 0 else jnp.where(head0, vt_r, vt)).astype(BF16)
            q = rope(qf[:, g * LANES:(g + 1) * LANES])
            q2 = jnp.concatenate([jnp.where(head0, q, 0.0), jnp.where(head0, 0.0, q)], axis=0).astype(BF16)
            scores = lax.dot_general(q2, k2, (((1,), (1,)), ((), ())), preferred_element_type=F32) * 64 ** -0.5
            scores = jnp.where(causal, scores, -jnp.inf)
            prob = jnp.exp(scores - jnp.max(scores, axis=-1, keepdims=True))
            prob = (prob / jnp.sum(prob, axis=-1, keepdims=True)).astype(BF16)
            both = dot(prob, v2)
            ctx[:, g * LANES:(g + 1) * LANES] = jnp.where(head0, both[:tokens], both[tokens:]).astype(BF16)

    e_lane = lax.broadcasted_iota(jnp.int32, (tokens, n_experts), 1) - me * n_local
    t_lane = lax.broadcasted_iota(jnp.int32, (n_experts, tokens), 1) < half

    def set_gates(c, par):
        if c == 0:
            gt = g_buf[0, par]
        elif c == 3:
            gt = g_buf[3, par]
        elif c == 1:
            gt = jnp.where(t_lane, g_buf[1, par], g_buf[2, par])
        else:
            gt = jnp.where(t_lane, g_buf[2, par], g_buf[1, par])
        gates_c = gt.T
        for e in range(n_local):
            gate = jnp.sum(jnp.where(e_lane == e, gates_c, 0.0), axis=-1, keepdims=True)
            gate = jnp.broadcast_to(gate, (tokens, LANES))
            for q in range(4):
                gate_b[e, place(c, par, q)] = gate[q * quarter:(q + 1) * quarter]

    def act(c, rows, e):
        x = x_buf[c, rows]
        used = jnp.concatenate([gate_b[e, rows]] * (COL // LANES), axis=1) > 0.0
        for n in range(exp_ff // COL):
            cols = slice(n * COL, (n + 1) * COL)
            z = silu(dot(x, v_eg[e, :, cols])) * dot(x, v_eu[e, :, cols])
            hb[rows, e * exp_ff + n * COL:e * exp_ff + (n + 1) * COL] = jnp.where(used, z, 0.0).astype(BF16)

    def down(c, rows, col_lo, col_hi):
        for n in range(col_lo // COL, col_hi // COL):
            cols = slice(n * COL, (n + 1) * COL)
            for e in range(n_local):
                y = dot(hb[rows, e * exp_ff:(e + 1) * exp_ff], v_ed[e, :, cols]).astype(BF16).astype(F32)
                y = y * jnp.concatenate([gate_b[e, rows]] * (COL // LANES), axis=1)
                p_buf[c, rows, cols] = y if e == 0 else p_buf[c, rows, cols] + y

    def down_cols(c):
        for n in range(N_P):
            down(c, both, n * model // N_P, (n + 1) * model // N_P)
            send(f'p{c}_{n}')

    def down_rows(c, n):
        down(c, slice(n * tokens, (n + 1) * tokens), 0, model)
        send(f'p{c}' + 'ab'[n])

    def add_cols(c):
        for n in range(N_P):
            recv(f'p{c}_{n}')
        p_buf[c, :tokens] = p_buf[c, :tokens] + pr_buf[c]

    def add_rows(c, n):
        recv(f'p{c}' + 'ab'[n])
        rows = slice(n * tokens, n * tokens + half)
        p_buf[c, rows] = p_buf[c, rows] + pr_buf[c, n * half:(n + 1) * half]

    def send_near(n):
        add_rows(1, n)
        send('i1' + 'ab'[n], 'i2' + 'ab'[n])

    def send_far(n):
        add_rows(3, n)
        send('o1' + 'ab'[n], 'o2' + 'ab'[n])

    def pass_on(n):
        recv('o1' + 'ab'[n], 'o2' + 'ab'[n])
        for q in (n, n + 2):
            p_buf[2, place(2, 0, q)] = p_buf[2, place(2, 0, q)] + tb[q * quarter:(q + 1) * quarter]
        send('w1' + 'ab'[n], 'w2' + 'ab'[n])

    def ffn_block(b, x):
        act_cols = slice(b * FF_BLOCK, (b + 1) * FF_BLOCK)
        for n in range(FF_BLOCK // COL):
            cols = slice(b * FF_BLOCK + n * COL, b * FF_BLOCK + (n + 1) * COL)
            z = silu(dot(x, v_fg[:, cols])) * dot(x, v_fu[:, cols])
            hb[:tokens, n * COL:(n + 1) * COL] = z.astype(BF16)
        h = hb[:tokens, :FF_BLOCK]
        for n in range(model // COL):
            cols = slice(n * COL, (n + 1) * COL)
            y = dot(h, v_fd[act_cols, cols])
            ffn_acc[:, cols] = y + (att[:, cols].astype(F32) if b == 0 else ffn_acc[:, cols])

    first, second, both = slice(0, tokens), slice(tokens, 2 * tokens), slice(0, 2 * tokens)
    attend(0)
    attend(1)
    attend(2)
    recv('a1a', 'a2a')
    send('f1a', 'f2a', 'd1a')
    recv('g1', 'g2')
    send('g3', 'gd1', 'gd2')
    attend(3)

    n_blk = ff_dim // 1024
    for b in range(n_blk):
        cols = pl.ds(b * 1024, 1024)
        load(f'fg{b}', ffn_gate.at[:, cols], v_fg.at[:, cols])
        load(f'fu{b}', ffn_up.at[:, cols], v_fu.at[:, cols])
        load(f'fd{b}', ffn_down.at[cols], v_fd.at[cols])

    for e in range(n_local):
        ready(f'eg{e}', f'eu{e}')
    recv('gd1', 'gd2', 'd1a')
    set_gates(1, 0)
    set_gates(1, 1)
    act(1, first, 0)
    recv('a1b', 'a2b')
    send('f1b', 'f2b', 'd1b', 'a3b', 'a4b')
    for e in range(1, n_local):
        act(1, first, e)
    for e in range(n_local):
        ready(f'ed{e}')
    down_rows(1, 0)
    recv('d1b')
    for e in range(n_local - 1):
        act(1, second, e)
    recv('f1a', 'f2a', 'g3')
    send('d3a', 'gd3')
    act(1, second, n_local - 1)
    send_near(0)
    down_rows(1, 1)
    recv('gd3', 'd3a')
    set_gates(3, 0)
    set_gates(3, 1)
    act(3, first, 0)
    act(3, first, 1)
    recv('f1b', 'f2b')
    send('d3b')
    act(3, first, 2)
    act(3, first, 3)
    send_near(1)
    down_rows(3, 0)
    recv('d3b', 'a3a', 'a4a', 'a3b', 'a4b')
    send('d2a', 'd2b')
    for e in range(n_local):
        act(3, second, e)
    send_far(0)
    down_rows(3, 1)
    recv('d2a')
    set_gates(2, 0)
    set_gates(2, 1)
    for e in range(n_local):
        act(2, first, e)
    send_far(1)
    down_rows(2, 0)
    recv('d2b')
    for e in range(n_local):
        act(2, second, e)
    add_rows(2, 0)
    pass_on(0)
    down_rows(2, 1)
    recv('d0', 'gd0')
    set_gates(0, 0)
    set_gates(0, 1)
    act(0, both, 0)
    act(0, both, 1)
    add_rows(2, 1)
    pass_on(1)
    act(0, both, 2)
    act(0, both, 3)
    down_cols(0)
    ready('wo', 'fn')
    att[...] = (v_hid[...].astype(F32) + dot(ctx[...], v_wo[...])).astype(BF16)
    normed_ffn = rms_rows(att[...], norm_row(v_fn))
    for b in range(n_blk):
        ready(f'fg{b}', f'fu{b}', f'fd{b}')
    for b in range(ff_dim // FF_BLOCK):
        ffn_block(b, normed_ffn)
    add_cols(0)
    recv('i1a', 'i2a', 'i1b', 'i2b')
    late = ('w1a', 'w2a', 'w1b', 'w2b')
    for name, copy in copies.items():
        if name not in late:
            copy.wait_send()
    total[...] = ffn_acc[...] + p_buf[0, :tokens] + near[...]
    for name in late:
        copies[name].wait_recv()
        copies[name].wait_send()


def solution(mesh):
    group = mesh.shape['ep']
    row_spec = P(('dp', 'ep'), None, None)
    vec_spec = P(None)
    mat_spec = P(None, None)
    cube_spec = P(None, None, None)
    expert_spec = P('ep', None, None)

    def per_device(hidden, expert_ids, slot_ids, attn_norm, w_query, w_key, w_value, w_out, ffn_norm, ffn_gate, ffn_up, ffn_down, moe_norm, w_router, exp_gate, exp_up, exp_down):
        n_seqs, seq_len, model = hidden.shape
        tokens = n_seqs * seq_len
        n_heads, head_dim = w_out.shape[0], w_out.shape[1]
        top_k = expert_ids.shape[-1]
        n_local, _, exp_ff = exp_gate.shape
        n_experts = w_router.shape[1]
        kv_dim = w_key.shape[1]
        assert n_seqs == 1 and group == 8 and head_dim == 64
        cos_t, sin_t = rope_tables(seq_len, head_dim)
        args = (hidden.reshape(tokens, model), expert_ids.reshape(tokens, top_k).T, attn_norm.reshape(-1, LANES),
                w_query, w_key, w_value, w_out.reshape(n_heads * head_dim, model), ffn_norm.reshape(-1, LANES),
                ffn_gate, ffn_up, ffn_down, moe_norm.reshape(-1, LANES), w_router.T, exp_gate, exp_up, exp_down,
                jnp.asarray(cos_t), jnp.asarray(sin_t))
        vmem = [pltpu.VMEM(a.shape, a.dtype) for a in args]
        scratch = vmem + [
            pltpu.VMEM((4, 2 * tokens, model), BF16),
            pltpu.VMEM((4, 2, n_experts, tokens), F32),
            pltpu.VMEM((4, 2 * tokens, model), F32),
            pltpu.VMEM((4, tokens, model), F32),
            pltpu.VMEM((tokens, model), F32),
            pltpu.VMEM((tokens, model), F32),
            pltpu.VMEM((tokens, n_heads * head_dim), F32),
            pltpu.VMEM((tokens, kv_dim), F32),
            pltpu.VMEM((tokens, kv_dim), F32),
            pltpu.VMEM((tokens, n_heads * head_dim), BF16),
            pltpu.VMEM((2 * tokens, n_local * exp_ff), BF16),
            pltpu.VMEM((n_local, 2 * tokens, LANES), F32),
            pltpu.VMEM((tokens, model), BF16),
            pltpu.VMEM((tokens, model), F32),
            pltpu.SemaphoreType.DMA((48,)),
            pltpu.SemaphoreType.DMA((64,)),
            pltpu.SemaphoreType.DMA((64,)),
        ]
        total, far = pl.pallas_call(
            functools.partial(kernel, group),
            out_shape=(pltpu.VMEM((tokens, model), F32), pltpu.VMEM((tokens, model), F32)),
            in_specs=[pl.BlockSpec(memory_space=pl.ANY)] * len(args),
            out_specs=(pl.BlockSpec(memory_space=pltpu.VMEM),) * 2,
            scratch_shapes=scratch,
            compiler_params=pltpu.CompilerParams(collective_id=0, has_side_effects=True, vmem_limit_bytes=VMEM_BYTES),
        )(*args)
        return (total + far).astype(BF16).reshape(n_seqs, seq_len, model)

    return jax.shard_map(per_device, mesh=mesh, in_specs=(row_spec, row_spec, row_spec, vec_spec, mat_spec, mat_spec, mat_spec, cube_spec, vec_spec, mat_spec, mat_spec, mat_spec, vec_spec, mat_spec, expert_spec, expert_spec, expert_spec), out_specs=row_spec, check_vma=False)
```

```python
import functools

import jax
import jax.numpy as jnp
import numpy as np
from jax import lax
from jax.experimental import pallas as pl
from jax.experimental.pallas import tpu as pltpu
from jax.sharding import PartitionSpec as P

RMS_EPS = 1e-6
ROPE_BASE = 10000.0
MESH = pl.DeviceIdType.MESH
F32, BF16 = jnp.float32, jnp.bfloat16
LANES = 128
FF_BLOCK = 1024
COL = 256
N_P = 2
VMEM_BYTES = 60 * 1024 * 1024


def rms_rows(row_vals, norm_scale):
    as_float = row_vals.astype(F32)
    inv_rms = lax.rsqrt(jnp.mean(as_float * as_float, axis=-1, keepdims=True) + RMS_EPS)
    return (as_float * inv_rms * norm_scale).astype(BF16)


def silu(z):
    half = 0.5 * z
    return half + half * jnp.tanh(half)


def dot(a, b):
    return jnp.dot(a, b, preferred_element_type=F32)


def rope_tables(seq_len, head_dim):
    half = head_dim // 2
    lane = np.arange(LANES)
    freq = ROPE_BASE ** (-2.0 * (lane % half) / head_dim)
    angle = np.arange(seq_len)[:, None] * freq[None, :]
    sign = np.where(lane % head_dim < half, -1.0, 1.0)
    return np.cos(angle).astype(np.float32), (np.sin(angle) * sign[None, :]).astype(np.float32)


def kernel(group, hidden, ids, attn_norm, w_query, w_key, w_value, w_out, ffn_norm, ffn_gate, ffn_up, ffn_down,
           moe_norm, w_router, exp_gate, exp_up, exp_down, cos_t, sin_t, total, far,
           v_hid, v_ids, v_an, v_wq, v_wk, v_wv, v_wo, v_fn, v_fg, v_fu, v_fd, v_mn, v_wr, v_eg, v_eu, v_ed, v_cos, v_sin,
           x_buf, g_buf, p_buf, pr_buf, tb, near, qf, kf, vf, ctx, hb, gate_b, att, ffn_acc,
           w_sem, s_sem, r_sem):
    tokens, model = v_hid.shape
    half, quarter = tokens // 2, tokens // 4
    n_local = v_eg.shape[0]
    exp_ff = v_eg.shape[2]
    ff_dim = v_fg.shape[1]
    n_experts = v_wr.shape[0]
    me = lax.axis_index('ep')
    partner = me + 1 - 2 * lax.rem(me, 2)
    right = lax.rem(me + 2, group)
    left = lax.rem(me + group - 2, group)

    loads = {}

    def load(name, src, dst):
        loads[name] = pltpu.make_async_copy(src, dst, w_sem.at[len(loads)])
        loads[name].start()

    def ready(*names):
        for name in names:
            loads[name].wait()

    copies = {}

    def remote(name, src, dst, device):
        k = len(copies)
        copies[name] = pltpu.make_async_remote_copy(
            src_ref=src, dst_ref=dst, send_sem=s_sem.at[k], recv_sem=r_sem.at[k],
            device_id={'ep': device}, device_id_type=MESH)

    def send(*names):
        for name in names:
            copies[name].start()

    def recv(*names):
        for name in names:
            copies[name].wait_recv()

    al, ot = pl.ds(0, tokens), pl.ds(tokens, tokens)

    def place(c, par, q):
        if c in (0, 2):
            return pl.ds(par * tokens + q * quarter, quarter)
        return pl.ds((q % 2) * tokens + par * half + (q // 2) * quarter, quarter)

    for name, c_src, q, c_dst, device in (
            ('a1a', 0, 0, 1, right), ('a1b', 0, 1, 1, right), ('a2a', 0, 2, 1, left), ('a2b', 0, 3, 1, left),
            ('a3a', 0, 2, 2, right), ('a3b', 0, 3, 2, right), ('a4a', 0, 0, 2, left), ('a4b', 0, 1, 2, left),
            ('f1a', 1, 0, 3, right), ('f1b', 1, 1, 3, right), ('f2a', 1, 2, 3, left), ('f2b', 1, 3, 3, left)):
        remote(name, x_buf.at[c_src, place(c_src, 0, q)], x_buf.at[c_dst, place(c_dst, 0, q)], device)
    p_cols = [pl.ds(n * model // N_P, model // N_P) for n in range(N_P)]
    for c in (0, 2):
        remote(f'd{c}', x_buf.at[c, al], x_buf.at[c, ot], partner)
        for n, cols in enumerate(p_cols):
            remote(f'p{c}_{n}', p_buf.at[c, ot, cols], pr_buf.at[c, :, cols], partner)
    for c in (1, 3):
        for n, part in enumerate('ab'):
            remote(f'd{c}{part}', x_buf.at[c, pl.ds(n * tokens, half)], x_buf.at[c, pl.ds(n * tokens + half, half)], partner)
            if c == 1:
                remote(f'p1{part}', p_buf.at[1, pl.ds(n * tokens + half, half)], pr_buf.at[1, pl.ds(n * half, half)], partner)
            else:
                for k, cols in enumerate(p_cols):
                    remote(f'p3{part}_{k}', p_buf.at[3, pl.ds(n * tokens + half, half), cols],
                           pr_buf.at[3, pl.ds(n * half, half), cols], partner)
    remote('g1', g_buf.at[0, 0], g_buf.at[1, 0], right)
    remote('g2', g_buf.at[0, 0], g_buf.at[2, 0], left)
    remote('g3', g_buf.at[1, 0], g_buf.at[3, 0], right)
    for c in range(4):
        remote(f'gd{c}', g_buf.at[c, 0], g_buf.at[c, 1], partner)
    for n, part in enumerate('ab'):
        for k, q, device in ((1, n, right), (2, n + 2, left)):
            rows = pl.ds(q * quarter, quarter)
            back = (q + 2) % 4
            remote(f'i{k}{part}', p_buf.at[1, place(1, 0, back)], near.at[pl.ds(back * quarter, quarter)], device)
            remote(f'o{k}{part}', p_buf.at[3, place(3, 0, q)], tb.at[rows], device)
            remote(f'w{k}{part}', p_buf.at[2, rows], far.at[rows], device)

    load('hid', hidden, v_hid)
    load('mn', moe_norm, v_mn)
    load('wr', w_router, v_wr)
    load('ids', ids, v_ids)
    load('an', attn_norm, v_an)
    load('wq', w_query, v_wq)
    load('wk', w_key, v_wk)
    load('wv', w_value, v_wv)
    load('fn', ffn_norm, v_fn)
    load('cos', cos_t, v_cos)
    load('sin', sin_t, v_sin)

    barrier = pltpu.get_barrier_semaphore()
    for peer in (partner, left, right):
        pl.semaphore_signal(barrier, inc=1, device_id={'ep': peer}, device_id_type=MESH)

    load('wo', w_out, v_wo)
    for e in range(n_local):
        load(f'eg{e}', exp_gate.at[e], v_eg.at[e])
        load(f'eu{e}', exp_up.at[e], v_eu.at[e])
    for e in range(n_local):
        load(f'ed{e}', exp_down.at[e], v_ed.at[e])

    def norm_row(ref):
        scale = ref[...].astype(F32)
        return jnp.concatenate([scale[r:r + 1] for r in range(scale.shape[0])], axis=1)

    ready('hid', 'mn')
    x_buf[0, :tokens] = rms_rows(v_hid[...], norm_row(v_mn))
    pl.semaphore_wait(barrier, 3)
    send('a1a', 'a2a', 'd0')

    ready('wr', 'ids')
    logits = lax.dot_general(v_wr[...], x_buf[0, :tokens], (((1,), (1,)), ((), ())), preferred_element_type=F32)
    expert_row = lax.broadcasted_iota(jnp.int32, logits.shape, 0)
    id_vals = v_ids[...]
    mask = expert_row == id_vals[0:1]
    for j in range(1, id_vals.shape[0]):
        mask = jnp.logical_or(mask, expert_row == id_vals[j:j + 1])
    top = jnp.max(jnp.where(mask, logits, -jnp.inf), axis=0, keepdims=True)
    powers = jnp.where(mask, jnp.exp(logits - top), 0.0)
    g_buf[0, 0] = powers / jnp.sum(powers, axis=0, keepdims=True)
    send('g1', 'g2', 'gd0', 'a1b', 'a2b', 'a3a', 'a4a')

    ready('an', 'wq', 'wk', 'wv', 'cos', 'sin')
    normed = rms_rows(v_hid[...], norm_row(v_an))
    qf[...] = dot(normed, v_wq[...])
    kf[...] = dot(normed, v_wk[...])
    vf[...] = dot(normed, v_wv[...])

    lane = lax.broadcasted_iota(jnp.int32, (tokens, LANES), 1)
    low_half = lax.rem(lane, 64) < 32
    head0 = lane < 64
    row = lax.rem(lax.broadcasted_iota(jnp.int32, (2 * tokens, tokens), 0), tokens)
    causal = row >= lax.broadcasted_iota(jnp.int32, (2 * tokens, tokens), 1)

    def rope(x):
        swapped = jnp.where(low_half, pltpu.roll(x, LANES - 32, 1), pltpu.roll(x, 32, 1))
        return x * v_cos[...] + swapped * v_sin[...]

    def attend(t):
        kt = rope(kf[:, t * LANES:(t + 1) * LANES])
        vt = vf[:, t * LANES:(t + 1) * LANES]
        kt_r, vt_r = pltpu.roll(kt, 64, 1), pltpu.roll(vt, 64, 1)
        for s in range(2):
            g = 2 * t + s
            k2 = (jnp.where(head0, kt, kt_r) if s == 0 else jnp.where(head0, kt_r, kt)).astype(BF16)
            v2 = (jnp.where(head0, vt, vt_r) if s == 0 else jnp.where(head0, vt_r, vt)).astype(BF16)
            q = rope(qf[:, g * LANES:(g + 1) * LANES])
            q2 = jnp.concatenate([jnp.where(head0, q, 0.0), jnp.where(head0, 0.0, q)], axis=0).astype(BF16)
            scores = lax.dot_general(q2, k2, (((1,), (1,)), ((), ())), preferred_element_type=F32) * 64 ** -0.5
            scores = jnp.where(causal, scores, -jnp.inf)
            prob = jnp.exp(scores - jnp.max(scores, axis=-1, keepdims=True))
            prob = (prob / jnp.sum(prob, axis=-1, keepdims=True)).astype(BF16)
            both = dot(prob, v2)
            ctx[:, g * LANES:(g + 1) * LANES] = jnp.where(head0, both[:tokens], both[tokens:]).astype(BF16)

    e_lane = lax.broadcasted_iota(jnp.int32, (tokens, n_experts), 1) - me * n_local
    t_lane = lax.broadcasted_iota(jnp.int32, (n_experts, tokens), 1) < half

    def set_gates(c, par):
        if c == 0:
            gt = g_buf[0, par]
        elif c == 3:
            gt = g_buf[3, par]
        elif c == 1:
            gt = jnp.where(t_lane, g_buf[1, par], g_buf[2, par])
        else:
            gt = jnp.where(t_lane, g_buf[2, par], g_buf[1, par])
        gates_c = gt.T
        for e in range(n_local):
            gate = jnp.sum(jnp.where(e_lane == e, gates_c, 0.0), axis=-1, keepdims=True)
            gate = jnp.broadcast_to(gate, (tokens, LANES))
            for q in range(4):
                gate_b[e, place(c, par, q)] = gate[q * quarter:(q + 1) * quarter]

    def act(c, rows, e):
        x = x_buf[c, rows]
        used = jnp.concatenate([gate_b[e, rows]] * (COL // LANES), axis=1) > 0.0
        for n in range(exp_ff // COL):
            cols = slice(n * COL, (n + 1) * COL)
            z = silu(dot(x, v_eg[e, :, cols])) * dot(x, v_eu[e, :, cols])
            hb[rows, e * exp_ff + n * COL:e * exp_ff + (n + 1) * COL] = jnp.where(used, z, 0.0).astype(BF16)

    def down(c, rows, col_lo, col_hi):
        for n in range(col_lo // COL, col_hi // COL):
            cols = slice(n * COL, (n + 1) * COL)
            for e in range(n_local):
                y = dot(hb[rows, e * exp_ff:(e + 1) * exp_ff], v_ed[e, :, cols]).astype(BF16).astype(F32)
                y = y * jnp.concatenate([gate_b[e, rows]] * (COL // LANES), axis=1)
                p_buf[c, rows, cols] = y if e == 0 else p_buf[c, rows, cols] + y

    def down_cols(c):
        for n in range(N_P):
            down(c, both, n * model // N_P, (n + 1) * model // N_P)
            send(*((f'p3a_{n}', f'p3b_{n}') if c == 3 else (f'p{c}_{n}',)))

    def down_rows(c, n):
        down(c, slice(n * tokens, (n + 1) * tokens), 0, model)
        send(f'p{c}' + 'ab'[n])

    def add_cols(c):
        for n in range(N_P):
            recv(f'p{c}_{n}')
        p_buf[c, :tokens] = p_buf[c, :tokens] + pr_buf[c]

    def add_rows(c, n):
        recv(*(('p1' + 'ab'[n],) if c == 1 else tuple('p3' + 'ab'[n] + f'_{k}' for k in range(N_P))))
        rows = slice(n * tokens, n * tokens + half)
        p_buf[c, rows] = p_buf[c, rows] + pr_buf[c, n * half:(n + 1) * half]

    def send_near(n):
        add_rows(1, n)
        send('i1' + 'ab'[n], 'i2' + 'ab'[n])

    def send_far(n):
        add_rows(3, n)
        send('o1' + 'ab'[n], 'o2' + 'ab'[n])

    def pass_on(n):
        recv('o1' + 'ab'[n], 'o2' + 'ab'[n])
        for q in (n, n + 2):
            rows = slice(q * quarter, (q + 1) * quarter)
            p_buf[2, rows] = p_buf[2, rows] + tb[rows]
        send('w1' + 'ab'[n], 'w2' + 'ab'[n])

    def ffn_block(b, x):
        act_cols = slice(b * FF_BLOCK, (b + 1) * FF_BLOCK)
        for n in range(FF_BLOCK // COL):
            cols = slice(b * FF_BLOCK + n * COL, b * FF_BLOCK + (n + 1) * COL)
            z = silu(dot(x, v_fg[:, cols])) * dot(x, v_fu[:, cols])
            hb[:tokens, n * COL:(n + 1) * COL] = z.astype(BF16)
        h = hb[:tokens, :FF_BLOCK]
        for n in range(model // COL):
            cols = slice(n * COL, (n + 1) * COL)
            y = dot(h, v_fd[act_cols, cols])
            ffn_acc[:, cols] = y + (att[:, cols].astype(F32) if b == 0 else ffn_acc[:, cols])

    first, second, both = slice(0, tokens), slice(tokens, 2 * tokens), slice(0, 2 * tokens)
    attend(0)
    attend(1)
    attend(2)
    recv('a1a', 'a2a')
    send('f1a', 'f2a', 'd1a')
    recv('g1', 'g2')
    send('g3', 'gd1', 'gd2')
    attend(3)
    ready('wo', 'fn')
    att[...] = (v_hid[...].astype(F32) + dot(ctx[...], v_wo[...])).astype(BF16)

    n_blk = ff_dim // 1024
    for b in range(n_blk):
        cols = pl.ds(b * 1024, 1024)
        load(f'fg{b}', ffn_gate.at[:, cols], v_fg.at[:, cols])
        load(f'fu{b}', ffn_up.at[:, cols], v_fu.at[:, cols])
        load(f'fd{b}', ffn_down.at[cols], v_fd.at[cols])

    for e in range(n_local):
        ready(f'eg{e}', f'eu{e}')
    recv('gd1', 'gd2', 'd1a')
    set_gates(1, 0)
    set_gates(1, 1)
    act(1, first, 0)
    recv('a1b', 'a2b')
    send('f1b', 'f2b', 'd1b', 'a3b', 'a4b')
    for e in range(1, n_local):
        act(1, first, e)
    for e in range(n_local):
        ready(f'ed{e}')
    down_rows(1, 0)
    recv('d1b')
    for e in range(n_local - 1):
        act(1, second, e)
    recv('f1a', 'f2a', 'g3')
    send('d3a', 'gd3')
    act(1, second, n_local - 1)
    send_near(0)
    recv('f1b', 'f2b')
    send('d3b')
    down_rows(1, 1)
    recv('gd3', 'd3a', 'd3b')
    set_gates(3, 0)
    set_gates(3, 1)
    act(3, both, 0)
    act(3, both, 1)
    send_near(1)
    recv('a3a', 'a3b', 'a4a', 'a4b')
    send('d2')
    act(3, both, 2)
    act(3, both, 3)
    down_cols(3)
    recv('d2')
    set_gates(2, 0)
    set_gates(2, 1)
    act(2, both, 0)
    act(2, both, 1)
    send_far(0)
    send_far(1)
    act(2, both, 2)
    act(2, both, 3)
    down_cols(2)
    recv('d0', 'gd0')
    set_gates(0, 0)
    set_gates(0, 1)
    act(0, both, 0)
    act(0, both, 1)
    add_cols(2)
    pass_on(0)
    act(0, both, 2)
    act(0, both, 3)
    down_cols(0)
    for b in range(n_blk):
        ready(f'fg{b}', f'fu{b}', f'fd{b}')
    pass_on(1)
    normed_ffn = rms_rows(att[...], norm_row(v_fn))
    for b in range(ff_dim // FF_BLOCK):
        ffn_block(b, normed_ffn)
    add_cols(0)
    recv('i1a', 'i2a', 'i1b', 'i2b')
    late = ('w1a', 'w2a', 'w1b', 'w2b')
    for name, copy in copies.items():
        if name not in late:
            copy.wait_send()
    total[...] = ffn_acc[...] + p_buf[0, :tokens] + near[...]
    for name in late:
        copies[name].wait_recv()
        copies[name].wait_send()


def solution(mesh):
    group = mesh.shape['ep']
    row_spec = P(('dp', 'ep'), None, None)
    vec_spec = P(None)
    mat_spec = P(None, None)
    cube_spec = P(None, None, None)
    expert_spec = P('ep', None, None)

    def per_device(hidden, expert_ids, slot_ids, attn_norm, w_query, w_key, w_value, w_out, ffn_norm, ffn_gate, ffn_up, ffn_down, moe_norm, w_router, exp_gate, exp_up, exp_down):
        n_seqs, seq_len, model = hidden.shape
        tokens = n_seqs * seq_len
        n_heads, head_dim = w_out.shape[0], w_out.shape[1]
        top_k = expert_ids.shape[-1]
        n_local, _, exp_ff = exp_gate.shape
        n_experts = w_router.shape[1]
        kv_dim = w_key.shape[1]
        assert n_seqs == 1 and group == 8 and head_dim == 64
        cos_t, sin_t = rope_tables(seq_len, head_dim)
        args = (hidden.reshape(tokens, model), expert_ids.reshape(tokens, top_k).T, attn_norm.reshape(-1, LANES),
                w_query, w_key, w_value, w_out.reshape(n_heads * head_dim, model), ffn_norm.reshape(-1, LANES),
                ffn_gate, ffn_up, ffn_down, moe_norm.reshape(-1, LANES), w_router.T, exp_gate, exp_up, exp_down,
                jnp.asarray(cos_t), jnp.asarray(sin_t))
        vmem = [pltpu.VMEM(a.shape, a.dtype) for a in args]
        scratch = vmem + [
            pltpu.VMEM((4, 2 * tokens, model), BF16),
            pltpu.VMEM((4, 2, n_experts, tokens), F32),
            pltpu.VMEM((4, 2 * tokens, model), F32),
            pltpu.VMEM((4, tokens, model), F32),
            pltpu.VMEM((tokens, model), F32),
            pltpu.VMEM((tokens, model), F32),
            pltpu.VMEM((tokens, n_heads * head_dim), F32),
            pltpu.VMEM((tokens, kv_dim), F32),
            pltpu.VMEM((tokens, kv_dim), F32),
            pltpu.VMEM((tokens, n_heads * head_dim), BF16),
            pltpu.VMEM((2 * tokens, n_local * exp_ff), BF16),
            pltpu.VMEM((n_local, 2 * tokens, LANES), F32),
            pltpu.VMEM((tokens, model), BF16),
            pltpu.VMEM((tokens, model), F32),
            pltpu.SemaphoreType.DMA((48,)),
            pltpu.SemaphoreType.DMA((64,)),
            pltpu.SemaphoreType.DMA((64,)),
        ]
        total, far = pl.pallas_call(
            functools.partial(kernel, group),
            out_shape=(pltpu.VMEM((tokens, model), F32), pltpu.VMEM((tokens, model), F32)),
            in_specs=[pl.BlockSpec(memory_space=pl.ANY)] * len(args),
            out_specs=(pl.BlockSpec(memory_space=pltpu.VMEM),) * 2,
            scratch_shapes=scratch,
            compiler_params=pltpu.CompilerParams(collective_id=0, has_side_effects=True, vmem_limit_bytes=VMEM_BYTES),
        )(*args)
        return (total + far).astype(BF16).reshape(n_seqs, seq_len, model)

    return jax.shard_map(per_device, mesh=mesh, in_specs=(row_spec, row_spec, row_spec, vec_spec, mat_spec, mat_spec, mat_spec, cube_spec, vec_spec, mat_spec, mat_spec, mat_spec, vec_spec, mat_spec, expert_spec, expert_spec, expert_spec), out_specs=row_spec, check_vma=False)
```

```python
import functools

import jax
import jax.numpy as jnp
import numpy as np
from jax import lax
from jax.experimental import pallas as pl
from jax.experimental.pallas import tpu as pltpu
from jax.sharding import PartitionSpec as P

RMS_EPS = 1e-6
ROPE_BASE = 10000.0
MESH = pl.DeviceIdType.MESH
F32, BF16 = jnp.float32, jnp.bfloat16
LANES = 128
FF_BLOCK = 512
COL = 256
N_P = 2
VMEM_BYTES = 60 * 1024 * 1024


def rms_rows(row_vals, norm_scale):
    as_float = row_vals.astype(F32)
    inv_rms = lax.rsqrt(jnp.mean(as_float * as_float, axis=-1, keepdims=True) + RMS_EPS)
    return (as_float * inv_rms * norm_scale).astype(BF16)


def silu(z):
    half = 0.5 * z
    return half + half * jnp.tanh(half)


def dot(a, b):
    return jnp.dot(a, b, preferred_element_type=F32)


def rope_tables(seq_len, head_dim):
    half = head_dim // 2
    lane = np.arange(LANES)
    freq = ROPE_BASE ** (-2.0 * (lane % half) / head_dim)
    angle = np.arange(seq_len)[:, None] * freq[None, :]
    sign = np.where(lane % head_dim < half, -1.0, 1.0)
    return np.cos(angle).astype(np.float32), (np.sin(angle) * sign[None, :]).astype(np.float32)


def kernel(group, hidden, ids, attn_norm, w_query, w_key, w_value, w_out, ffn_norm, ffn_gate, ffn_up, ffn_down,
           moe_norm, w_router, exp_gate, exp_up, exp_down, cos_t, sin_t, total, far,
           v_hid, v_ids, v_an, v_wq, v_wk, v_wv, v_wo, v_fn, v_fg, v_fu, v_fd, v_mn, v_wr, v_eg, v_eu, v_ed, v_cos, v_sin,
           x_buf, g_buf, p_buf, pr_buf, tb, near, qf, kf, vf, ctx, hb, gate_b, att, ffn_acc,
           w_sem, s_sem, r_sem):
    tokens, model = v_hid.shape
    half, quarter = tokens // 2, tokens // 4
    n_local = v_eg.shape[0]
    exp_ff = v_eg.shape[2]
    ff_dim = v_fg.shape[1]
    n_experts = v_wr.shape[0]
    me = lax.axis_index('ep')
    partner = me + 1 - 2 * lax.rem(me, 2)
    right = lax.rem(me + 2, group)
    left = lax.rem(me + group - 2, group)

    loads = {}

    def load(name, src, dst):
        loads[name] = pltpu.make_async_copy(src, dst, w_sem.at[len(loads)])
        loads[name].start()

    def ready(*names):
        for name in names:
            loads[name].wait()

    copies = {}

    def remote(name, src, dst, device):
        k = len(copies)
        copies[name] = pltpu.make_async_remote_copy(
            src_ref=src, dst_ref=dst, send_sem=s_sem.at[k], recv_sem=r_sem.at[k],
            device_id={'ep': device}, device_id_type=MESH)

    def send(*names):
        for name in names:
            copies[name].start()

    def recv(*names):
        for name in names:
            copies[name].wait_recv()

    al, ot = pl.ds(0, tokens), pl.ds(tokens, tokens)

    def place(c, par, q):
        if c in (0, 2):
            return pl.ds(par * tokens + q * quarter, quarter)
        return pl.ds((q % 2) * tokens + par * half + (q // 2) * quarter, quarter)

    for name, c_src, q, c_dst, device in (
            ('a1a', 0, 0, 1, right), ('a1b', 0, 1, 1, right), ('a2a', 0, 2, 1, left), ('a2b', 0, 3, 1, left),
            ('a3a', 0, 2, 2, right), ('a3b', 0, 3, 2, right), ('a4a', 0, 0, 2, left), ('a4b', 0, 1, 2, left),
            ('f1a', 1, 0, 3, right), ('f1b', 1, 1, 3, right), ('f2a', 1, 2, 3, left), ('f2b', 1, 3, 3, left)):
        remote(name, x_buf.at[c_src, place(c_src, 0, q)], x_buf.at[c_dst, place(c_dst, 0, q)], device)
    p_cols = [pl.ds(n * model // N_P, model // N_P) for n in range(N_P)]
    for c in (0, 2):
        remote(f'd{c}', x_buf.at[c, al], x_buf.at[c, ot], partner)
        for n, cols in enumerate(p_cols):
            remote(f'p{c}_{n}', p_buf.at[c, ot, cols], pr_buf.at[c, :, cols], partner)
    for c in (1, 3):
        for n, part in enumerate('ab'):
            remote(f'd{c}{part}', x_buf.at[c, pl.ds(n * tokens, half)], x_buf.at[c, pl.ds(n * tokens + half, half)], partner)
            remote(f'p{c}{part}', p_buf.at[c, pl.ds(n * tokens + half, half)], pr_buf.at[c, pl.ds(n * half, half)], partner)
    remote('g1', g_buf.at[0, 0], g_buf.at[1, 0], right)
    remote('g2', g_buf.at[0, 0], g_buf.at[2, 0], left)
    remote('g3', g_buf.at[1, 0], g_buf.at[3, 0], right)
    for c in range(4):
        remote(f'gd{c}', g_buf.at[c, 0], g_buf.at[c, 1], partner)
    for n, part in enumerate('ab'):
        for k, q, device in ((1, n, right), (2, n + 2, left)):
            rows = pl.ds(q * quarter, quarter)
            back = (q + 2) % 4
            remote(f'i{k}{part}', p_buf.at[1, place(1, 0, back)], near.at[pl.ds(back * quarter, quarter)], device)
            remote(f'o{k}{part}', p_buf.at[3, place(3, 0, q)], tb.at[rows], device)
            remote(f'w{k}{part}', p_buf.at[2, rows], far.at[rows], device)

    load('hid', hidden, v_hid)
    load('mn', moe_norm, v_mn)
    load('wr', w_router, v_wr)
    load('ids', ids, v_ids)
    load('an', attn_norm, v_an)
    load('wq', w_query, v_wq)
    load('wk', w_key, v_wk)
    load('wv', w_value, v_wv)
    load('fn', ffn_norm, v_fn)
    load('cos', cos_t, v_cos)
    load('sin', sin_t, v_sin)

    barrier = pltpu.get_barrier_semaphore()
    for peer in (partner, left, right):
        pl.semaphore_signal(barrier, inc=1, device_id={'ep': peer}, device_id_type=MESH)

    load('wo', w_out, v_wo)
    for e in range(n_local):
        load(f'eg{e}', exp_gate.at[e], v_eg.at[e])
        load(f'eu{e}', exp_up.at[e], v_eu.at[e])
    for e in range(n_local):
        load(f'ed{e}', exp_down.at[e], v_ed.at[e])

    def norm_row(ref):
        scale = ref[...].astype(F32)
        return jnp.concatenate([scale[r:r + 1] for r in range(scale.shape[0])], axis=1)

    ready('hid', 'mn')
    x_buf[0, :tokens] = rms_rows(v_hid[...], norm_row(v_mn))
    pl.semaphore_wait(barrier, 3)
    send('a1a', 'a2a', 'd0')

    ready('wr', 'ids')
    logits = lax.dot_general(v_wr[...], x_buf[0, :tokens], (((1,), (1,)), ((), ())), preferred_element_type=F32)
    expert_row = lax.broadcasted_iota(jnp.int32, logits.shape, 0)
    id_vals = v_ids[...]
    mask = expert_row == id_vals[0:1]
    for j in range(1, id_vals.shape[0]):
        mask = jnp.logical_or(mask, expert_row == id_vals[j:j + 1])
    top = jnp.max(jnp.where(mask, logits, -jnp.inf), axis=0, keepdims=True)
    powers = jnp.where(mask, jnp.exp(logits - top), 0.0)
    g_buf[0, 0] = powers / jnp.sum(powers, axis=0, keepdims=True)
    send('g1', 'g2', 'gd0', 'a1b', 'a2b', 'a3a', 'a4a')

    ready('an', 'wq', 'wk', 'wv', 'cos', 'sin')
    normed = rms_rows(v_hid[...], norm_row(v_an))
    qf[...] = dot(normed, v_wq[...])
    kf[...] = dot(normed, v_wk[...])
    vf[...] = dot(normed, v_wv[...])

    lane = lax.broadcasted_iota(jnp.int32, (tokens, LANES), 1)
    low_half = lax.rem(lane, 64) < 32
    head0 = lane < 64
    row = lax.rem(lax.broadcasted_iota(jnp.int32, (2 * tokens, tokens), 0), tokens)
    causal = row >= lax.broadcasted_iota(jnp.int32, (2 * tokens, tokens), 1)

    def rope(x):
        swapped = jnp.where(low_half, pltpu.roll(x, LANES - 32, 1), pltpu.roll(x, 32, 1))
        return x * v_cos[...] + swapped * v_sin[...]

    def attend(t):
        kt = rope(kf[:, t * LANES:(t + 1) * LANES])
        vt = vf[:, t * LANES:(t + 1) * LANES]
        kt_r, vt_r = pltpu.roll(kt, 64, 1), pltpu.roll(vt, 64, 1)
        for s in range(2):
            g = 2 * t + s
            k2 = (jnp.where(head0, kt, kt_r) if s == 0 else jnp.where(head0, kt_r, kt)).astype(BF16)
            v2 = (jnp.where(head0, vt, vt_r) if s == 0 else jnp.where(head0, vt_r, vt)).astype(BF16)
            q = rope(qf[:, g * LANES:(g + 1) * LANES])
            q2 = jnp.concatenate([jnp.where(head0, q, 0.0), jnp.where(head0, 0.0, q)], axis=0).astype(BF16)
            scores = lax.dot_general(q2, k2, (((1,), (1,)), ((), ())), preferred_element_type=F32) * 64 ** -0.5
            scores = jnp.where(causal, scores, -jnp.inf)
            prob = jnp.exp(scores - jnp.max(scores, axis=-1, keepdims=True))
            prob = (prob / jnp.sum(prob, axis=-1, keepdims=True)).astype(BF16)
            both = dot(prob, v2)
            ctx[:, g * LANES:(g + 1) * LANES] = jnp.where(head0, both[:tokens], both[tokens:]).astype(BF16)

    e_lane = lax.broadcasted_iota(jnp.int32, (tokens, n_experts), 1) - me * n_local
    t_lane = lax.broadcasted_iota(jnp.int32, (n_experts, tokens), 1) < half

    def set_gates(c, par):
        if c == 0:
            gt = g_buf[0, par]
        elif c == 3:
            gt = g_buf[3, par]
        elif c == 1:
            gt = jnp.where(t_lane, g_buf[1, par], g_buf[2, par])
        else:
            gt = jnp.where(t_lane, g_buf[2, par], g_buf[1, par])
        gates_c = gt.T
        for e in range(n_local):
            gate = jnp.sum(jnp.where(e_lane == e, gates_c, 0.0), axis=-1, keepdims=True)
            gate = jnp.broadcast_to(gate, (tokens, LANES))
            for q in range(4):
                gate_b[e, place(c, par, q)] = gate[q * quarter:(q + 1) * quarter]

    def act(c, rows, e):
        x = x_buf[c, rows]
        used = jnp.concatenate([gate_b[e, rows]] * (COL // LANES), axis=1) > 0.0
        for n in range(exp_ff // COL):
            cols = slice(n * COL, (n + 1) * COL)
            z = silu(dot(x, v_eg[e, :, cols])) * dot(x, v_eu[e, :, cols])
            hb[rows, e * exp_ff + n * COL:e * exp_ff + (n + 1) * COL] = jnp.where(used, z, 0.0).astype(BF16)

    def down(c, rows, col_lo, col_hi):
        for n in range(col_lo // COL, col_hi // COL):
            cols = slice(n * COL, (n + 1) * COL)
            for e in range(n_local):
                y = dot(hb[rows, e * exp_ff:(e + 1) * exp_ff], v_ed[e, :, cols]).astype(BF16).astype(F32)
                y = y * jnp.concatenate([gate_b[e, rows]] * (COL // LANES), axis=1)
                p_buf[c, rows, cols] = y if e == 0 else p_buf[c, rows, cols] + y

    def down_cols(c):
        for n in range(N_P):
            down(c, both, n * model // N_P, (n + 1) * model // N_P)
            send(f'p{c}_{n}')

    def down_rows(c, n):
        down(c, slice(n * tokens, (n + 1) * tokens), 0, model)
        send(f'p{c}' + 'ab'[n])

    def add_cols(c):
        for n in range(N_P):
            recv(f'p{c}_{n}')
        p_buf[c, :tokens] = p_buf[c, :tokens] + pr_buf[c]

    def add_rows(c, n):
        recv(f'p{c}' + 'ab'[n])
        rows = slice(n * tokens, n * tokens + half)
        p_buf[c, rows] = p_buf[c, rows] + pr_buf[c, n * half:(n + 1) * half]

    def send_near(n):
        add_rows(1, n)
        send('i1' + 'ab'[n], 'i2' + 'ab'[n])

    def send_far(n):
        add_rows(3, n)
        send('o1' + 'ab'[n], 'o2' + 'ab'[n])

    def pass_on(n):
        recv('o1' + 'ab'[n], 'o2' + 'ab'[n])
        for q in (n, n + 2):
            rows = slice(q * quarter, (q + 1) * quarter)
            p_buf[2, rows] = p_buf[2, rows] + tb[rows]
        send('w1' + 'ab'[n], 'w2' + 'ab'[n])

    def ffn_block(b, x):
        act_cols = slice(b * FF_BLOCK, (b + 1) * FF_BLOCK)
        for n in range(FF_BLOCK // COL):
            cols = slice(b * FF_BLOCK + n * COL, b * FF_BLOCK + (n + 1) * COL)
            z = silu(dot(x, v_fg[:, cols])) * dot(x, v_fu[:, cols])
            hb[:tokens, n * COL:(n + 1) * COL] = z.astype(BF16)
        h = hb[:tokens, :FF_BLOCK]
        for n in range(model // COL):
            cols = slice(n * COL, (n + 1) * COL)
            y = dot(h, v_fd[act_cols, cols])
            ffn_acc[:, cols] = y + (att[:, cols].astype(F32) if b == 0 else ffn_acc[:, cols])

    first, second, both = slice(0, tokens), slice(tokens, 2 * tokens), slice(0, 2 * tokens)
    attend(0)
    attend(1)
    attend(2)
    recv('a1a', 'a2a')
    send('f1a', 'f2a', 'd1a')
    recv('g1', 'g2')
    send('g3', 'gd1', 'gd2')
    attend(3)
    ready('wo', 'fn')
    att[...] = (v_hid[...].astype(F32) + dot(ctx[...], v_wo[...])).astype(BF16)

    n_blk = ff_dim // 1024
    for b in range(n_blk):
        cols = pl.ds(b * 1024, 1024)
        load(f'fg{b}', ffn_gate.at[:, cols], v_fg.at[:, cols])
        load(f'fu{b}', ffn_up.at[:, cols], v_fu.at[:, cols])
        load(f'fd{b}', ffn_down.at[cols], v_fd.at[cols])

    for e in range(n_local):
        ready(f'eg{e}', f'eu{e}')
    recv('gd1', 'gd2', 'd1a')
    set_gates(1, 0)
    set_gates(1, 1)
    act(1, first, 0)
    recv('a1b', 'a2b')
    send('f1b', 'f2b', 'd1b', 'a3b', 'a4b')
    for e in range(1, n_local):
        act(1, first, e)
    for e in range(n_local):
        ready(f'ed{e}')
    down_rows(1, 0)
    recv('d1b')
    for e in range(n_local - 1):
        act(1, second, e)
    recv('f1a', 'f2a', 'g3')
    send('d3a', 'gd3')
    act(1, second, n_local - 1)
    send_near(0)
    down_rows(1, 1)
    recv('gd3', 'd3a')
    set_gates(3, 0)
    set_gates(3, 1)
    act(3, first, 0)
    act(3, first, 1)
    recv('f1b', 'f2b')
    send('d3b')
    act(3, first, 2)
    act(3, first, 3)
    send_near(1)
    down_rows(3, 0)
    recv('d3b', 'a3a', 'a3b', 'a4a', 'a4b')
    send('d2')
    for e in range(n_local):
        act(3, second, e)
    send_far(0)
    down_rows(3, 1)
    recv('d2')
    set_gates(2, 0)
    set_gates(2, 1)
    act(2, both, 0)
    act(2, both, 1)
    send_far(1)
    act(2, both, 2)
    act(2, both, 3)
    down_cols(2)
    recv('d0', 'gd0')
    set_gates(0, 0)
    set_gates(0, 1)
    act(0, both, 0)
    act(0, both, 1)
    add_cols(2)
    pass_on(0)
    act(0, both, 2)
    act(0, both, 3)
    down_cols(0)
    for b in range(n_blk):
        ready(f'fg{b}', f'fu{b}', f'fd{b}')
    pass_on(1)
    normed_ffn = rms_rows(att[...], norm_row(v_fn))
    for b in range(ff_dim // FF_BLOCK):
        ffn_block(b, normed_ffn)
    add_cols(0)
    recv('i1a', 'i2a', 'i1b', 'i2b')
    late = ('w1a', 'w2a', 'w1b', 'w2b')
    for name, copy in copies.items():
        if name not in late:
            copy.wait_send()
    total[...] = ffn_acc[...] + p_buf[0, :tokens] + near[...]
    for name in late:
        copies[name].wait_recv()
        copies[name].wait_send()


def solution(mesh):
    group = mesh.shape['ep']
    row_spec = P(('dp', 'ep'), None, None)
    vec_spec = P(None)
    mat_spec = P(None, None)
    cube_spec = P(None, None, None)
    expert_spec = P('ep', None, None)

    def per_device(hidden, expert_ids, slot_ids, attn_norm, w_query, w_key, w_value, w_out, ffn_norm, ffn_gate, ffn_up, ffn_down, moe_norm, w_router, exp_gate, exp_up, exp_down):
        n_seqs, seq_len, model = hidden.shape
        tokens = n_seqs * seq_len
        n_heads, head_dim = w_out.shape[0], w_out.shape[1]
        top_k = expert_ids.shape[-1]
        n_local, _, exp_ff = exp_gate.shape
        n_experts = w_router.shape[1]
        kv_dim = w_key.shape[1]
        assert n_seqs == 1 and group == 8 and head_dim == 64
        cos_t, sin_t = rope_tables(seq_len, head_dim)
        args = (hidden.reshape(tokens, model), expert_ids.reshape(tokens, top_k).T, attn_norm.reshape(-1, LANES),
                w_query, w_key, w_value, w_out.reshape(n_heads * head_dim, model), ffn_norm.reshape(-1, LANES),
                ffn_gate, ffn_up, ffn_down, moe_norm.reshape(-1, LANES), w_router.T, exp_gate, exp_up, exp_down,
                jnp.asarray(cos_t), jnp.asarray(sin_t))
        vmem = [pltpu.VMEM(a.shape, a.dtype) for a in args]
        scratch = vmem + [
            pltpu.VMEM((4, 2 * tokens, model), BF16),
            pltpu.VMEM((4, 2, n_experts, tokens), F32),
            pltpu.VMEM((4, 2 * tokens, model), F32),
            pltpu.VMEM((4, tokens, model), F32),
            pltpu.VMEM((tokens, model), F32),
            pltpu.VMEM((tokens, model), F32),
            pltpu.VMEM((tokens, n_heads * head_dim), F32),
            pltpu.VMEM((tokens, kv_dim), F32),
            pltpu.VMEM((tokens, kv_dim), F32),
            pltpu.VMEM((tokens, n_heads * head_dim), BF16),
            pltpu.VMEM((2 * tokens, n_local * exp_ff), BF16),
            pltpu.VMEM((n_local, 2 * tokens, LANES), F32),
            pltpu.VMEM((tokens, model), BF16),
            pltpu.VMEM((tokens, model), F32),
            pltpu.SemaphoreType.DMA((48,)),
            pltpu.SemaphoreType.DMA((64,)),
            pltpu.SemaphoreType.DMA((64,)),
        ]
        total, far = pl.pallas_call(
            functools.partial(kernel, group),
            out_shape=(pltpu.VMEM((tokens, model), F32), pltpu.VMEM((tokens, model), F32)),
            in_specs=[pl.BlockSpec(memory_space=pl.ANY)] * len(args),
            out_specs=(pl.BlockSpec(memory_space=pltpu.VMEM),) * 2,
            scratch_shapes=scratch,
            compiler_params=pltpu.CompilerParams(collective_id=0, has_side_effects=True, vmem_limit_bytes=VMEM_BYTES),
        )(*args)
        return (total + far).astype(BF16).reshape(n_seqs, seq_len, model)

    return jax.shard_map(per_device, mesh=mesh, in_specs=(row_spec, row_spec, row_spec, vec_spec, mat_spec, mat_spec, mat_spec, cube_spec, vec_spec, mat_spec, mat_spec, mat_spec, vec_spec, mat_spec, expert_spec, expert_spec, expert_spec), out_specs=row_spec, check_vma=False)
```
